32 devices in a mesh: heads: 4 (over x, core), ctx: 8 (over z, y).
Axes of the slice: x: 2, y: 2, z: 4, core: 2. Of those that a mesh axis runs over, the one named last changes fastest.
Arguments:
- queries: bfloat16 [1536, 2048], P('ctx', 'heads'), may hold values from -6 to 6
- key_states: bfloat16 [1536, 512], P('ctx', 'heads'), may hold values from -6 to 6
- value_states: bfloat16 [1536, 512], P('ctx', 'heads'), may hold values from -6 to 6
- attention_out: bfloat16 [1536, 2048], P('ctx', 'heads'), may hold values from -2 to 2
- out_grad: bfloat16 [1536, 2048], P('ctx', 'heads'), may hold values from -6 to 6
- log_sum_exp: float32 [16, 1536], P('heads', 'ctx'), may hold values from 0 to 16, as said below
- block_counts: int32 [8], replicated, may hold values from 1 to 3, as said below
- w_query: bfloat16 [4096, 2048], P(None, 'heads'), may hold values from -0.09375 to 0.09375
- w_key: bfloat16 [4096, 512], P(None, 'heads'), may hold values from -0.09375 to 0.09375
- w_value: bfloat16 [4096, 512], P(None, 'heads'), may hold values from -0.09375 to 0.09375
Outputs:
- input_grad: bfloat16 [1536, 4096], P('ctx', 'heads')
- key_grad: float32 [1536, 512], P('ctx', 'heads')
- value_grad: float32 [1536, 512], P('ctx', 'heads')
The draws below stay inside these ranges and needn't reach their ends.
Inputs may be any that keep to these rules, and one draw needn't show every extreme that they name: `block_counts`: one entry equals 3. `log_sum_exp`: finite offsets of each row's scores.
All inputs are finite; a program needn't handle non-finite values.
Results may differ from the reference program's by a relative error of at most 0.0063.
Values may be sent and summed in bfloat16 or wider, within the bound.
A program may use at most 128 MiB of HBM per device.

```python
import math
import jax
import jax.numpy as jnp
from jax import lax

D_MODEL = 4096
HEAD_DIM = 128
GROUP = 4
CAP = 192
BLOCK = 64
KV_HEADS = 4
TOKENS_CAP = 1536
N_CTX = 8


def shared_counts(key):
    count_key = jax.random.fold_in(key, 101)
    pick_key = jax.random.fold_in(key, 202)
    counts = jax.random.randint(count_key, (N_CTX,), 1, CAP // BLOCK + 1, dtype=jnp.int32)
    chosen = jax.random.randint(pick_key, (), 0, N_CTX, dtype=jnp.int32)
    return jnp.where(jnp.arange(N_CTX, dtype=jnp.int32) == chosen, CAP // BLOCK, counts).astype(jnp.int32)


def draw_block_counts(key, part):
    return shared_counts(key)


def draw_log_sum_exp(key, part):
    counts = shared_counts(key)
    lengths = counts * BLOCK
    offsets = jnp.cumsum(lengths) - lengths
    row_index = jnp.arange(CAP * N_CTX, dtype=jnp.int32)
    device = row_index // CAP
    within = row_index - device * CAP
    position = offsets[device] + within
    visible_keys = (position + 1).astype(jnp.float32)
    noise_key = jax.random.fold_in(key, 303)
    base = jax.random.uniform(noise_key, (KV_HEADS * GROUP, CAP * N_CTX), jnp.float32, 0.3, 1.2)
    return jnp.log(visible_keys)[None, :] + base


def steps_of(rng, shape, split, least, high):
    level = 1.0
    for dim, blocks in split:
        steps = jax.random.uniform(jax.random.fold_in(jax.random.fold_in(rng, 6), dim), (blocks,), jnp.float32, least / len(split), high / len(split))
        level = level * jnp.repeat(jnp.exp(steps), shape[dim] // blocks).reshape((-1,) + (1,) * (len(shape) - 1 - dim))
    return level


def bell_draw(rng, shape, spread, reach, pieces=(), held_as=jnp.bfloat16):
    entries = jax.random.normal(rng, shape, jnp.float32) * spread
    if len(pieces) > 0:
        entries = steps_of(rng, shape, pieces, -0.22, 0.18) * entries
    return jnp.clip(entries, min=-reach, max=reach).astype(held_as)


def setup_inputs(seed: int = 0) -> dict:
    splits = jax.random.split(jax.random.key(seed), 11)
    queries = bell_draw(splits[0], (TOKENS_CAP, KV_HEADS * GROUP * HEAD_DIM), 1.0, 6.0, ((0, 8), (1, 4)))
    key_states = bell_draw(splits[1], (TOKENS_CAP, KV_HEADS * HEAD_DIM), 1.0, 6.0, ((0, 8), (1, 4)))
    value_states = bell_draw(splits[2], (TOKENS_CAP, KV_HEADS * HEAD_DIM), 1.0, 6.0, ((0, 8), (1, 4)))
    attention_out = bell_draw(splits[3], (TOKENS_CAP, KV_HEADS * GROUP * HEAD_DIM), 0.3, 2.0, ((0, 8), (1, 4)))
    out_grad = bell_draw(splits[4], (TOKENS_CAP, KV_HEADS * GROUP * HEAD_DIM), 1.0, 6.0, ((0, 8), (1, 4)))
    log_sum_exp = draw_log_sum_exp(jax.random.fold_in(splits[10], 71), 0)
    block_counts = draw_block_counts(jax.random.fold_in(splits[10], 71), 0)
    w_query = bell_draw(splits[7], (D_MODEL, KV_HEADS * GROUP * HEAD_DIM), D_MODEL ** -0.5, 0.09375, ((1, 4),))
    w_key = bell_draw(splits[8], (D_MODEL, KV_HEADS * HEAD_DIM), D_MODEL ** -0.5, 0.09375, ((1, 4),))
    w_value = bell_draw(splits[9], (D_MODEL, KV_HEADS * HEAD_DIM), D_MODEL ** -0.5, 0.09375, ((1, 4),))
    return dict(queries=queries, key_states=key_states, value_states=value_states, attention_out=attention_out, out_grad=out_grad, log_sum_exp=log_sum_exp, block_counts=block_counts, w_query=w_query, w_key=w_key, w_value=w_value)


def slot_table(block_counts):
    lengths = (block_counts * BLOCK).astype(jnp.int32)
    offsets = (jnp.cumsum(lengths) - lengths).astype(jnp.int32)
    row_index = jnp.arange(CAP * N_CTX, dtype=jnp.int32)
    device = row_index // CAP
    within = row_index - device * CAP
    position = offsets[device] + within
    live = within < lengths[device]
    return (position, live)

def reference(queries, key_states, value_states, attention_out, out_grad, log_sum_exp, block_counts, w_query, w_key, w_value):
    total_rows = CAP * N_CTX
    score_scale = 1.0 / math.sqrt(HEAD_DIM)
    position, live = slot_table(block_counts)
    query_block = math.gcd(total_rows, 512)
    width = GROUP * HEAD_DIM
    query_parts = []
    key_parts = []
    value_parts = []
    for head_num in range(KV_HEADS):
        query_h = queries[:, head_num * width:(head_num + 1) * width].reshape(total_rows, GROUP, HEAD_DIM)
        grad_h = out_grad[:, head_num * width:(head_num + 1) * width].reshape(total_rows, GROUP, HEAD_DIM)
        output_h = attention_out[:, head_num * width:(head_num + 1) * width].reshape(total_rows, GROUP, HEAD_DIM)
        key_h = key_states[:, head_num * HEAD_DIM:(head_num + 1) * HEAD_DIM].astype(jnp.float32)
        value_h = value_states[:, head_num * HEAD_DIM:(head_num + 1) * HEAD_DIM].astype(jnp.float32)
        norm_h = log_sum_exp[head_num * GROUP:(head_num + 1) * GROUP]
        delta_h = lax.optimization_barrier(jnp.sum(grad_h.astype(jnp.float32) * output_h.astype(jnp.float32), axis=2))

        def step_block(totals, block_num):
            key_acc, value_acc = totals
            begin_row = (block_num * query_block).astype(jnp.int32)
            query_blk = lax.dynamic_slice_in_dim(query_h, begin_row, query_block, 0).astype(jnp.float32)
            grad_blk = lax.dynamic_slice_in_dim(grad_h, begin_row, query_block, 0).astype(jnp.float32)
            norm_blk = lax.dynamic_slice_in_dim(norm_h, begin_row, query_block, 1)
            delta_blk = lax.dynamic_slice_in_dim(delta_h, begin_row, query_block, 0)
            query_pos = lax.dynamic_slice_in_dim(position, begin_row, query_block, 0)
            query_live = lax.dynamic_slice_in_dim(live, begin_row, query_block, 0)
            scores = jnp.einsum('qgd,kd->gqk', query_blk, key_h) * score_scale
            visible = query_live[:, None] & live[None, :] & (position[None, :] <= query_pos[:, None])
            probability = jnp.where(visible[None], jnp.exp(scores - norm_blk[:, :, None]), 0.0)
            prob_grad = jnp.einsum('qgd,kd->gqk', grad_blk, value_h)
            score_grad = probability * (prob_grad - delta_blk.T[:, :, None])
            prob_b = probability.astype(jnp.bfloat16).astype(jnp.float32)
            grad_b = score_grad.astype(jnp.bfloat16).astype(jnp.float32)
            query_terms = score_scale * jnp.einsum('gqk,kd->qgd', grad_b, key_h)
            key_acc = key_acc + score_scale * jnp.einsum('gqk,qgd->kd', grad_b, query_blk)
            value_acc = value_acc + jnp.einsum('gqk,qgd->kd', prob_b, grad_blk)
            return ((key_acc, value_acc), query_terms)
        zero_keys = jnp.zeros((total_rows, HEAD_DIM), jnp.float32)
        (key_acc, value_acc), grad_blocks = lax.scan(step_block, (zero_keys, zero_keys), jnp.arange(total_rows // query_block, dtype=jnp.int32))
        query_parts.append(grad_blocks.reshape(total_rows, width))
        key_parts.append(key_acc)
        value_parts.append(value_acc)
    query_grad = jnp.concatenate(query_parts, axis=1)
    key_grad = jnp.concatenate(key_parts, axis=1)
    value_grad = jnp.concatenate(value_parts, axis=1)
    input_grad = jnp.dot(query_grad.astype(jnp.bfloat16), w_query.T, preferred_element_type=jnp.float32)
    input_grad = input_grad + jnp.dot(key_grad.astype(jnp.bfloat16), w_key.T, preferred_element_type=jnp.float32)
    input_grad = input_grad + jnp.dot(value_grad.astype(jnp.bfloat16), w_value.T, preferred_element_type=jnp.float32)
    return (input_grad.astype(jnp.bfloat16), key_grad, value_grad)
```

```python
import functools
import math

import jax
import jax.numpy as jnp
from jax import lax
from jax.experimental import pallas as pl
from jax.experimental.pallas import tpu as pltpu
from jax.sharding import PartitionSpec as P

BLOCK = 64
LOG2E = math.log2(math.e)
F32 = jnp.float32
BF16 = jnp.bfloat16
NT = (((1,), (1,)), ((), ()))
TN = (((0,), (0,)), ((), ()))


def dot(a, b, dims=(((1,), (0,)), ((), ()))):
    return lax.dot_general(a, b, dims, preferred_element_type=F32)


def row_blocks(np, ns):
    plan = []
    for r in range(np):
        if r == 0:
            plan.append(((0, 1), (1, 1), (2, ns - 2)))
        elif r == np - 1:
            plan.append(((0, ns - 2), (ns - 2, 1), (ns - 1, 1)))
        else:
            plan.append(((0, ns // 2), (ns // 2, ns - ns // 2)))
    return plan


def kernel(
    zs, nx, ns, nb,
    q_hbm, k_hbm, v_hbm, o_hbm, do_hbm, lse_hbm, cnt_hbm, wq_hbm, wk_hbm, wv_hbm,
    out_ref, dk_ref, dv_ref,
    cnt_ref, own, qd, o_ref, lse_ref, pair_qd, wq, wkv, qs, dos, stats, dqt,
    dq_own, dq_send, dq_recv, gq, gkv, acc, kv, part, fsend, frcv, keep, hold, csend, crcv, tsend, trcv, xsend, xrcv,
    in_sem, w_sem, own_send, kv_recv, swap_send, swap_recv, f_send, f_recv,
    c_send, c_recv, t_send, t_recv, x_send, x_recv,
):
    cap, dim = own.shape[1:]
    group = qd.shape[2] // dim
    np = dq_send.shape[0]
    half = cap // np
    scale = 1.0 / math.sqrt(dim)
    plan = row_blocks(np, ns)
    first = [sum(len(p) for p in plan[:r]) for r in range(np)]
    me = lax.axis_index("ctx")
    y = lax.rem(me, 2)
    z = lax.div(me, 2)
    pair = me + 1 - 2 * y
    h = lax.axis_index("heads")
    core = lax.rem(h, 2)
    x = lax.div(h, 2)
    other = h + 1 - 2 * core
    across = [2 * lax.rem(x + dx, nx) + core for dx in range(nx)]

    loads = [
        pltpu.make_async_copy(src, dst, in_sem.at[i])
        for src, dst, i in (
            (k_hbm, own.at[0], 0), (v_hbm, own.at[1], 0), (q_hbm, qd.at[0], 1), (do_hbm, qd.at[1], 1),
            (o_hbm, o_ref, 2), (lse_hbm, lse_ref, 3), (cnt_hbm, cnt_ref, 4),
        )
    ]
    for copy in loads:
        copy.start()
    w_copies = [
        pltpu.make_async_copy(wq_hbm, wq, w_sem.at[0]),
        pltpu.make_async_copy(wk_hbm, wkv.at[:, pl.ds(0, dim)], w_sem.at[1]),
        pltpu.make_async_copy(wv_hbm, wkv.at[:, pl.ds(dim, dim)], w_sem.at[1]),
    ]

    def remote(src, dst, send, recv, **device):
        return pltpu.make_async_remote_copy(
            src_ref=src, dst_ref=dst, send_sem=send, recv_sem=recv,
            device_id=device, device_id_type=pl.DeviceIdType.MESH,
        )

    barrier = pltpu.get_barrier_semaphore()

    def greet(**device):
        pl.semaphore_signal(
            barrier, inc=1, device_id=device, device_id_type=pl.DeviceIdType.MESH
        )

    def greet_line(z2, _):
        @pl.when(z2 != z)
        def _():
            greet(ctx=2 * z2 + y)
        return 0

    lax.fori_loop(0, zs, greet_line, 0)
    greet(ctx=pair)
    greet(heads=other)
    for dx in range(1, nx):
        greet(heads=across[dx])
    pltpu.make_async_copy(own, own, in_sem.at[0]).wait()
    pltpu.make_async_copy(qd, qd, in_sem.at[1]).wait()
    for copy in loads[4:]:
        copy.wait()
    for copy in w_copies:
        copy.start()
    with jax.named_scope("barrier"):
        pl.semaphore_wait(barrier, zs + nx)

    def own_copy(z2):
        return remote(own, kv.at[z], own_send.at[z2], kv_recv.at[z], ctx=2 * z2 + y)

    pair_own_copy = remote(own, kv.at[zs], own_send.at[zs], kv_recv.at[zs], ctx=pair)

    def arrived(z1):
        remote(kv.at[z1], kv.at[z1], own_send.at[z1], kv_recv.at[z1], ctx=pair).wait_recv()

    swap_qd = remote(qd, pair_qd, swap_send.at[0], swap_recv.at[0], ctx=pair)
    swap_stats = remote(stats.at[0], stats.at[1], swap_send.at[1], swap_recv.at[1], ctx=pair)

    def swap_dq(r):
        return remote(dq_send.at[r], dq_recv.at[r], swap_send.at[2], swap_recv.at[2 + r], ctx=pair)

    def fin_copy(r, z1):
        return remote(
            fsend.at[z1, r], frcv.at[z, r], f_send.at[z1], f_recv.at[z, r], ctx=2 * z1 + y
        )

    def pair_fin(r):
        return remote(
            fsend.at[zs, r], frcv.at[zs, r], f_send.at[zs], f_recv.at[zs, r], ctx=pair
        )

    def fin_wait(r, z2):
        remote(
            fsend.at[z2, r], frcv.at[z2, r], f_send.at[z2], f_recv.at[z2, r], ctx=pair
        ).wait_recv()

    swapping = z > 0

    @pl.when(swapping)
    def _():
        swap_qd.start()

    @pl.when((z == 0) & (y == 0))
    def _():
        pair_own_copy.start()

    def push_own(i, _):
        z2 = zs - 1 - i

        @pl.when(z2 > z)
        def _():
            own_copy(z2).start()
        return 0

    lax.fori_loop(0, zs, push_own, 0)

    lane = lax.broadcasted_iota(jnp.int32, (1, group * cap), 1)
    row = lax.rem(lane, cap)
    alive = row < cnt_ref[me] * BLOCK
    prod = jnp.concatenate(
        [
            qd[1, :, g * dim:(g + 1) * dim].astype(F32) * o_ref[:, g * dim:(g + 1) * dim].astype(F32)
            for g in range(group)
        ],
        axis=0,
    )
    stats[0, 1:2] = lax.dot_general(
        jnp.ones((8, dim), F32), prod, NT,
        preferred_element_type=F32, precision=lax.Precision.HIGHEST,
    )[0:1]
    lse_row = jnp.concatenate([lse_ref[g:g + 1, :] for g in range(group)], axis=1)
    stats[0, 0:1] = jnp.where(alive, lse_row * LOG2E, 1e30)

    def stack(who, src):
        for g in range(group):
            cols = slice(g * dim, (g + 1) * dim)
            qs[who, g * cap:(g + 1) * cap, :] = src[0, :, cols]
            dos[who, g * cap:(g + 1) * cap, :] = src[1, :, cols]

    stack(0, qd)

    @pl.when(swapping)
    def _():
        swap_stats.start()

    key_row = lax.broadcasted_iota(jnp.int32, (cap, group * cap), 0)

    def tile(who, key, value, b, diagonal):
        scores = dot(key, qs[who], NT)
        prob_grad = dot(value, dos[who], NT)
        visible = key_row < cnt_ref[b] * BLOCK
        if diagonal:
            visible = visible & (key_row <= row)
        prob = jnp.where(visible, jnp.exp2(scores * (scale * LOG2E) - stats[who, 0:1]), 0.0)
        grad = (prob * (prob_grad - stats[who, 1:2])).astype(BF16)
        d_value = dot(prob.astype(BF16), dos[who])
        d_key = dot(grad, qs[who])
        terms = dot(key, grad, TN)
        if diagonal:
            dqt[who] = terms
        else:
            dqt[who] += terms
        return d_key, d_value

    with jax.named_scope("diag"):
        d_key, d_value = tile(0, own[0], own[1], me, True)
        acc[0] = d_key
        acc[1] = d_value

    def own_step(z1, _):
        @pl.when((z1 < z) | ((z1 == zs) & (z == 0) & (y == 1)))
        def _():
            with jax.named_scope("wait_kv"):
                arrived(z1)
            with jax.named_scope("own_tile"):
                b = jnp.where(z1 == zs, pair, 2 * z1 + y)
                d_key, d_value = tile(0, kv[z1, 0], kv[z1, 1], b, False)
                part[z1, 0] = d_key
                part[z1, 1] = d_value
        return 0

    lax.fori_loop(0, zs + 1, own_step, 0)
    dq_own[...] = jnp.transpose(dqt[0])

    def ship(z1, d_key, d_value):
        for r in range(np):
            fsend[z1, r, 0] = d_key[r * half:(r + 1) * half].astype(BF16)
            fsend[z1, r, 1] = d_value[r * half:(r + 1) * half].astype(BF16)

    @pl.when((z == 0) & (y == 1))
    def _():
        ship(zs, part[zs, 0], part[zs, 1])
        for r in range(np):
            pair_fin(r).start()

    @pl.when(z == 0)
    def _():
        dq_recv[...] = jnp.zeros_like(dq_recv)

    def later(r):
        def step(z1, _):
            @pl.when(z1 < z)
            def _():
                fin_copy(r, z1).start()
            return 0
        lax.fori_loop(0, zs, step, 0)

    @pl.when(swapping)
    def _():
        dqt[1] = jnp.zeros_like(dqt[1])
        with jax.named_scope("wait_swap"):
            swap_qd.wait_recv()
            swap_stats.wait_recv()
        stack(1, pair_qd)

        def pair_step(z1, _):
            @pl.when(z1 < z)
            def _():
                with jax.named_scope("pair_tile"):
                    d_key, d_value = tile(1, kv[z1, 0], kv[z1, 1], 2 * z1 + y, False)
                    ship(z1, part[z1, 0] + d_key, part[z1, 1] + d_value)
                fin_copy(0, z1).start()
            return 0

        lax.fori_loop(0, zs, pair_step, 0)

        @pl.when(y == 0)
        def _():
            with jax.named_scope("pair_own"):
                d_key, d_value = tile(1, own[0], own[1], me, False)
                acc[0] += d_key
                acc[1] += d_value

        pair_dq = jnp.transpose(dqt[1]).astype(BF16)
        for r in range(np):
            for g in range(group):
                dq_send[r, g] = pair_dq[g * cap + r * half:g * cap + (r + 1) * half]
            swap_dq(r).start()
        later(1)

    w_copies[0].wait()
    pltpu.make_async_copy(wkv, wkv, w_sem.at[1]).wait()
    width = hold.shape[2] * nb // ns

    def whole(owner, s, n, rows):
        cols = pl.ds(pl.multiple_of((owner * ns + s) * width, width), n * width)
        return dot(gq[rows, :], wq[cols, :], NT) + dot(gkv[rows, :], wkv[cols, :], NT)

    def chip_copy(b):
        return remote(csend.at[b], crcv.at[b], c_send.at[0], c_recv.at[b], heads=other)

    def near_copy(dx, r, i):
        at = (dx - 1, r, pl.ds(*plan[r][i]))
        return remote(
            tsend.at[at], trcv.at[at], t_send.at[0], t_recv.at[dx - 1, first[r] + i], heads=other
        )

    def cross_copy(dx, r, i):
        at = (dx - 1, r, pl.ds(*plan[r][i]))
        return remote(
            xsend.at[at], xrcv.at[at], x_send.at[0], x_recv.at[dx - 1, first[r] + i], heads=across[dx]
        )

    for r in range(np):
        rows = slice(r * half, (r + 1) * half)

        def collect(i, _):
            z2 = zs - i

            @pl.when(((z2 > z) & (z2 < zs)) | ((z2 == zs) & (z == 0) & (y == 0)))
            def _():
                fin_wait(r, z2)
                acc[:, rows, :] += frcv[z2, r].astype(F32)
            return 0

        with jax.named_scope("wait_dq"):
            @pl.when(swapping)
            def _():
                swap_dq(r).wait_recv()
        if r == 0:
            for rr in range(2, np):
                later(rr)
        for g in range(group):
            total = dq_own[g * cap + r * half:g * cap + (r + 1) * half, :] + dq_recv[r, g].astype(F32)
            gq[rows, g * dim:(g + 1) * dim] = (total * scale).astype(BF16)
        with jax.named_scope("collect"):
            lax.fori_loop(0, zs + 1, collect, 0)
        key_total = acc[0, rows, :] * scale
        value_total = acc[1, rows, :]
        dk_ref[rows, :] = key_total
        dv_ref[rows, :] = value_total
        gkv[rows, 0:dim] = key_total.astype(BF16)
        gkv[rows, dim:2 * dim] = value_total.astype(BF16)
        for dx in range(1, nx):
            with jax.named_scope("near"):
                for i, (s, n) in enumerate(plan[r]):
                    terms = whole(across[dx] + 1 - 2 * core, s, n, rows).astype(BF16)
                    for j in range(n):
                        tsend[dx - 1, r, s + j] = terms[:, j * width:(j + 1) * width]
                    near_copy(dx, r, i).start()
            with jax.named_scope("cross"):
                for i, (s, n) in enumerate(plan[r]):
                    terms = whole(across[dx], s, n, rows)
                    for j in range(n):
                        keep[s + j] = terms[:, j * width:(j + 1) * width]
                    near_copy(dx, r, i).wait_recv()
                    for j in range(s, s + n):
                        xsend[dx - 1, r, j] = (keep[j] + trcv[dx - 1, r, j].astype(F32)).astype(BF16)
                    cross_copy(dx, r, i).start()
    everything = slice(0, cap)
    per = ns // nb
    with jax.named_scope("chip_proj"):
        for b in range(nb):
            csend[b] = whole(other, b * per, per, everything).astype(BF16)
            chip_copy(b).start()
        for b in range(nb):
            hold[b] = whole(h, b * per, per, everything)
    with jax.named_scope("chip_wait"):
        for b in range(nb):
            chip_copy(b).wait_recv()
            hold[b] += crcv[b].astype(F32)
    for r in range(np):
        rows = slice(r * half, (r + 1) * half)
        for i, (s, n) in enumerate(plan[r]):
            for dx in range(1, nx):
                with jax.named_scope("wait_cross"):
                    cross_copy(dx, r, i).wait_recv()
            for j in range(s, s + n):
                total = hold[j // per, rows, (j % per) * width:(j % per + 1) * width]
                for dx in range(1, nx):
                    total = total + xrcv[dx - 1, r, j].astype(F32)
                out_ref[rows, j * width:(j + 1) * width] = total.astype(BF16)

    with jax.named_scope("drain"):
        @pl.when(swapping)
        def _():
            swap_qd.wait_send()
            swap_stats.wait_send()
            remote(dq_send, dq_recv, swap_send.at[2], swap_recv.at[2], ctx=pair).wait_send()

        def fins_sent(z1):
            remote(fsend.at[z1], frcv.at[z1], f_send.at[z1], f_recv.at[z1, 0], ctx=pair).wait_send()

        def drain(z2, _):
            @pl.when(z2 > z)
            def _():
                own_copy(z2).wait_send()

            @pl.when(z2 < z)
            def _():
                fins_sent(z2)
            return 0

        lax.fori_loop(0, zs, drain, 0)

        @pl.when((z == 0) & (y == 0))
        def _():
            pair_own_copy.wait_send()

        @pl.when((z == 0) & (y == 1))
        def _():
            fins_sent(zs)

        remote(csend, crcv, c_send.at[0], c_recv.at[0], heads=other).wait_send()
        remote(tsend, trcv, t_send.at[0], t_recv.at[0, 0], heads=other).wait_send()
        for dx in range(1, nx):
            remote(
                xsend.at[dx - 1], xrcv.at[dx - 1], x_send.at[0], x_recv.at[dx - 1, 0], heads=across[dx]
            ).wait_send()


def emit(a, b, c, a_hbm, b_hbm, c_hbm, sem):
    copies = [
        pltpu.make_async_copy(src, dst, sem.at[i])
        for i, (src, dst) in enumerate(((a, a_hbm), (b, b_hbm), (c, c_hbm)))
    ]
    for copy in copies:
        copy.start()
    for copy in copies:
        copy.wait()


def on_device(
    n, nh, queries, key_states, value_states, attention_out, out_grad, log_sum_exp, block_counts,
    w_query, w_key, w_value,
):
    zs, nx, ns, nb = n // 2, nh // 2, 4, 2
    cap, dim = key_states.shape
    width = queries.shape[1]
    rows = width // dim * cap
    model = w_query.shape[0]
    mine = model // nh
    chunk = mine // ns
    vmem = pl.BlockSpec(memory_space=pltpu.VMEM)
    half = BLOCK
    np = cap // half
    blocks = sum(len(p) for p in row_blocks(np, ns))
    hbm = pl.BlockSpec(memory_space=pltpu.HBM)
    dma = pltpu.SemaphoreType.DMA
    results = pl.pallas_call(
        functools.partial(kernel, zs, nx, ns, nb),
        out_shape=(
            jax.ShapeDtypeStruct((cap, mine), BF16),
            jax.ShapeDtypeStruct((cap, dim), F32),
            jax.ShapeDtypeStruct((cap, dim), F32),
        ),
        in_specs=[hbm] * 10,
        out_specs=(vmem, vmem, vmem),
        scratch_shapes=[
            pltpu.SMEM(block_counts.shape, jnp.int32),
            pltpu.VMEM((2, cap, dim), BF16),
            pltpu.VMEM((2, cap, width), BF16),
            pltpu.VMEM((cap, width), BF16),
            pltpu.VMEM(log_sum_exp.shape, F32),
            pltpu.VMEM((2, cap, width), BF16),
            pltpu.VMEM((model, width), BF16),
            pltpu.VMEM((model, 2 * dim), BF16),
            pltpu.VMEM((2, rows, dim), BF16),
            pltpu.VMEM((2, rows, dim), BF16),
            pltpu.VMEM((2, 2, rows), F32),
            pltpu.VMEM((2, dim, rows), F32),
            pltpu.VMEM((rows, dim), F32),
            pltpu.VMEM((np, width // dim, half, dim), BF16),
            pltpu.VMEM((np, width // dim, half, dim), BF16),
            pltpu.VMEM((cap, width), BF16),
            pltpu.VMEM((cap, 2 * dim), BF16),
            pltpu.VMEM((2, cap, dim), F32),
            pltpu.VMEM((zs + 1, 2, cap, dim), BF16),
            pltpu.VMEM((zs + 1, 2, cap, dim), F32),
            pltpu.VMEM((zs + 1, np, 2, half, dim), BF16),
            pltpu.VMEM((zs + 1, np, 2, half, dim), BF16),
            pltpu.VMEM((ns, half, chunk), F32),
            pltpu.VMEM((nb, cap, mine // nb), F32),
            pltpu.VMEM((nb, cap, mine // nb), BF16),
            pltpu.VMEM((nb, cap, mine // nb), BF16),
            pltpu.VMEM((nx - 1, np, ns, half, chunk), BF16),
            pltpu.VMEM((nx - 1, np, ns, half, chunk), BF16),
            pltpu.VMEM((nx - 1, np, ns, half, chunk), BF16),
            pltpu.VMEM((nx - 1, np, ns, half, chunk), BF16),
            dma((5,)),
            dma((2,)),
            dma((zs + 1,)),
            dma((zs + 1,)),
            dma((3,)),
            dma((2 + np,)),
            dma((zs + 1,)),
            dma((zs + 1, np)),
            dma((1,)),
            dma((nb,)),
            dma((1,)),
            dma((nx - 1, blocks)),
            dma((1,)),
            dma((nx - 1, blocks)),
        ],
        compiler_params=pltpu.CompilerParams(
            collective_id=0, has_side_effects=True, vmem_limit_bytes=52 * 1024 * 1024
        ),
    )(
        *(
            pltpu.with_memory_space_constraint(a, pltpu.HBM)
            for a in (
                queries, key_states, value_states, attention_out, out_grad, log_sum_exp,
                block_counts, w_query, w_key, w_value,
            )
        )
    )
    return pl.pallas_call(
        emit,
        out_shape=tuple(jax.ShapeDtypeStruct(a.shape, a.dtype) for a in results),
        in_specs=[vmem] * 3,
        out_specs=(hbm,) * 3,
        scratch_shapes=[dma((3,))],
    )(*(pltpu.with_memory_space_constraint(a, pltpu.VMEM) for a in results))


def solution(mesh):
    return jax.shard_map(
        functools.partial(on_device, mesh.shape["ctx"], mesh.shape["heads"]),
        mesh=mesh,
        in_specs=(
            P("ctx", "heads"),
            P("ctx", "heads"),
            P("ctx", "heads"),
            P("ctx", "heads"),
            P("ctx", "heads"),
            P("heads", "ctx"),
            P(),
            P(None, "heads"),
            P(None, "heads"),
            P(None, "heads"),
        ),
        out_specs=(P("ctx", "heads"), P("ctx", "heads"), P("ctx", "heads")),
        check_vma=False,
    )
```

```python
import functools
import math

import jax
import jax.numpy as jnp
from jax import lax
from jax.experimental import pallas as pl
from jax.experimental.pallas import tpu as pltpu
from jax.sharding import PartitionSpec as P

BLOCK = 64
LOG2E = math.log2(math.e)
F32 = jnp.float32
BF16 = jnp.bfloat16
NT = (((1,), (1,)), ((), ()))
TN = (((0,), (0,)), ((), ()))


def dot(a, b, dims=(((1,), (0,)), ((), ()))):
    return lax.dot_general(a, b, dims, preferred_element_type=F32)


def row_blocks(np, ns):
    plan = []
    for r in range(np):
        if r == 0:
            plan.append(((0, 1), (1, 1), (2, ns - 2)))
        elif r == np - 1:
            plan.append(((0, ns - 2), (ns - 2, 1), (ns - 1, 1)))
        else:
            plan.append(((0, ns // 2), (ns // 2, ns - ns // 2)))
    return plan


def kernel(
    zs, nx, ns,
    q_hbm, k_hbm, v_hbm, o_hbm, do_hbm, lse_hbm, cnt_hbm, wq_hbm, wk_hbm, wv_hbm,
    out_ref, dk_ref, dv_ref,
    cnt_ref, own, qd, o_ref, lse_ref, pair_qd, w, qs, dos, stats, dqt,
    dq_own, dq_send, dq_recv, gs, acc, kv, part, fsend, frcv, hold, xsend, xrcv,
    in_sem, w_sem, w_send, w_recv, own_send, kv_recv, swap_send, swap_recv, f_send, f_recv,
    g_send, g_recv, x_send, x_recv, turn,
):
    cap, dim = own.shape[1:]
    group = qd.shape[2] // dim
    np = dq_send.shape[0]
    half = cap // np
    scale = 1.0 / math.sqrt(dim)
    plan = row_blocks(np, ns)
    first = [sum(len(p) for p in plan[:r]) for r in range(np)]
    me = lax.axis_index("ctx")
    y = lax.rem(me, 2)
    z = lax.div(me, 2)
    pair = me + 1 - 2 * y
    h = lax.axis_index("heads")
    core = lax.rem(h, 2)
    x = lax.div(h, 2)
    other = h + 1 - 2 * core
    across = [2 * lax.rem(x + dx, nx) + core for dx in range(nx)]

    loads = [
        pltpu.make_async_copy(src, dst, in_sem.at[i])
        for src, dst, i in (
            (k_hbm, own.at[0], 0), (v_hbm, own.at[1], 0), (q_hbm, qd.at[0], 1), (do_hbm, qd.at[1], 1),
            (o_hbm, o_ref, 2), (lse_hbm, lse_ref, 3), (cnt_hbm, cnt_ref, 4),
        )
    ]
    for copy in loads:
        copy.start()
    def remote(src, dst, send, recv, **device):
        return pltpu.make_async_remote_copy(
            src_ref=src, dst_ref=dst, send_sem=send, recv_sem=recv,
            device_id=device, device_id_type=pl.DeviceIdType.MESH,
        )

    mine = w.shape[1] // nx
    wide = qd.shape[2]
    weights = ((wq_hbm, 0, wide), (wk_hbm, wide, dim), (wv_hbm, wide + dim, dim))

    def w_rows(owner, src):
        return src.at[pl.ds(pl.multiple_of(owner * mine, mine), mine), :]

    w_loads = [
        pltpu.make_async_copy(
            w_rows(across[dx], src), w.at[0, pl.ds(dx * mine, mine), pl.ds(at, size)], w_sem.at[0]
        )
        for dx in range(nx)
        for src, at, size in weights
    ]
    w_shares = [
        remote(
            w_rows(across[dx] + 1 - 2 * core, src), w.at[1, pl.ds(dx * mine, mine), pl.ds(at, size)],
            w_send.at[0], w_recv.at[0], heads=other,
        )
        for dx in range(nx)
        for src, at, size in weights
    ]
    barrier = pltpu.get_barrier_semaphore()

    def greet(**device):
        pl.semaphore_signal(
            barrier, inc=1, device_id=device, device_id_type=pl.DeviceIdType.MESH
        )

    def greet_line(z2, _):
        @pl.when(z2 != z)
        def _():
            greet(ctx=2 * z2 + y)
        return 0

    lax.fori_loop(0, zs, greet_line, 0)
    greet(ctx=pair)
    greet(heads=other)
    for dx in range(1, nx):
        greet(heads=across[dx])
    pltpu.make_async_copy(own, own, in_sem.at[0]).wait()
    pltpu.make_async_copy(qd, qd, in_sem.at[1]).wait()
    for copy in loads[4:]:
        copy.wait()
    for copy in w_loads:
        copy.start()
    with jax.named_scope("barrier"):
        pl.semaphore_wait(barrier, zs + nx)

    def own_copy(z2):
        return remote(own, kv.at[z], own_send.at[z2], kv_recv.at[z], ctx=2 * z2 + y)

    pair_own_copy = remote(own, kv.at[zs], own_send.at[zs], kv_recv.at[zs], ctx=pair)

    def arrived(z1):
        remote(kv.at[z1], kv.at[z1], own_send.at[z1], kv_recv.at[z1], ctx=pair).wait_recv()

    swap_q, swap_do = (
        remote(qd.at[i], pair_qd.at[i], swap_send.at[3 * i], swap_recv.at[(2 + np) * i], ctx=pair)
        for i in range(2)
    )
    swap_stats = remote(stats.at[0], stats.at[1], swap_send.at[1], swap_recv.at[1], ctx=pair)

    def swap_dq(r):
        return remote(dq_send.at[r], dq_recv.at[r], swap_send.at[2], swap_recv.at[2 + r], ctx=pair)

    def fin_copy(r, z1):
        return remote(
            fsend.at[z1, r], frcv.at[z, r], f_send.at[z1], f_recv.at[z, r], ctx=2 * z1 + y
        )

    def pair_fin(r):
        return remote(
            fsend.at[zs, r], frcv.at[zs, r], f_send.at[zs], f_recv.at[zs, r], ctx=pair
        )

    def fin_wait(r, z2):
        remote(
            fsend.at[z2, r], frcv.at[z2, r], f_send.at[z2], f_recv.at[z2, r], ctx=pair
        ).wait_recv()

    swapping = z > 0
    early = swapping & (core == 0)
    late = swapping & (core == 1)

    @pl.when(early)
    def _():
        swap_q.start()
        swap_do.start()

    @pl.when((z == 0) & (y == 0))
    def _():
        pair_own_copy.start()

    def push_own(i, _):
        z2 = zs - 1 - i

        @pl.when(z2 > z)
        def _():
            own_copy(z2).start()
        return 0

    lax.fori_loop(0, zs, push_own, 0)

    lane = lax.broadcasted_iota(jnp.int32, (1, group * cap), 1)
    row = lax.rem(lane, cap)
    alive = row < cnt_ref[me] * BLOCK
    prod = jnp.concatenate(
        [
            qd[1, :, g * dim:(g + 1) * dim].astype(F32) * o_ref[:, g * dim:(g + 1) * dim].astype(F32)
            for g in range(group)
        ],
        axis=0,
    )
    stats[0, 1:2] = lax.dot_general(
        jnp.ones((8, dim), F32), prod, NT,
        preferred_element_type=F32, precision=lax.Precision.HIGHEST,
    )[0:1]
    lse_row = jnp.concatenate([lse_ref[g:g + 1, :] for g in range(group)], axis=1)
    stats[0, 0:1] = jnp.where(alive, lse_row * LOG2E, 1e30)

    def stack(who, src):
        for g in range(group):
            cols = slice(g * dim, (g + 1) * dim)
            qs[who, g * cap:(g + 1) * cap, :] = src[0, :, cols]
            dos[who, g * cap:(g + 1) * cap, :] = src[1, :, cols]

    stack(0, qd)

    @pl.when(swapping)
    def _():
        swap_stats.start()

    key_row = lax.broadcasted_iota(jnp.int32, (cap, group * cap), 0)

    def tile(who, key, value, b, diagonal):
        scores = dot(key, qs[who], NT)
        prob_grad = dot(value, dos[who], NT)
        visible = key_row < cnt_ref[b] * BLOCK
        if diagonal:
            visible = visible & (key_row <= row)
        prob = jnp.where(visible, jnp.exp2(scores * (scale * LOG2E) - stats[who, 0:1]), 0.0)
        grad = (prob * (prob_grad - stats[who, 1:2])).astype(BF16)
        d_value = dot(prob.astype(BF16), dos[who])
        d_key = dot(grad, qs[who])
        terms = dot(key, grad, TN)
        if diagonal:
            dqt[who] = terms
        else:
            dqt[who] += terms
        return d_key, d_value

    with jax.named_scope("diag"):
        d_key, d_value = tile(0, own[0], own[1], me, True)
        acc[0] = d_key
        acc[1] = d_value

    for copy in w_shares:
        copy.start()

    @pl.when(early)
    def _():
        with jax.named_scope("hand_over"):
            swap_q.wait_send()
            pl.semaphore_signal(
                turn, inc=1, device_id={"heads": other}, device_id_type=pl.DeviceIdType.MESH
            )

    @pl.when(late)
    def _():
        with jax.named_scope("my_turn"):
            pl.semaphore_wait(turn, 1)
            swap_q.start()
            swap_do.start()

    def ship(z1, d_key, d_value):
        for r in range(np):
            fsend[z1, r, 0] = d_key[r * half:(r + 1) * half].astype(BF16)
            fsend[z1, r, 1] = d_value[r * half:(r + 1) * half].astype(BF16)

    def later(r):
        def step(z1, _):
            @pl.when(z1 < z)
            def _():
                fin_copy(r, z1).start()
            return 0
        lax.fori_loop(0, zs, step, 0)

    def swapped():
        dqt[1] = jnp.zeros_like(dqt[1])
        with jax.named_scope("wait_swap"):
            swap_q.wait_recv()
            swap_do.wait_recv()
            swap_stats.wait_recv()
        stack(1, pair_qd)

    def pair_tile(z1):
        with jax.named_scope("pair_tile"):
            d_key, d_value = tile(1, kv[z1, 0], kv[z1, 1], 2 * z1 + y, False)
            ship(z1, part[z1, 0] + d_key, part[z1, 1] + d_value)
        fin_copy(0, z1).start()

    pl.when(early)(swapped)

    def own_step(z1, _):
        @pl.when((z1 < z) | ((z1 == zs) & (z == 0) & (y == 1)))
        def _():
            with jax.named_scope("wait_kv"):
                arrived(z1)
            with jax.named_scope("own_tile"):
                b = jnp.where(z1 == zs, pair, 2 * z1 + y)
                d_key, d_value = tile(0, kv[z1, 0], kv[z1, 1], b, False)
                part[z1, 0] = d_key
                part[z1, 1] = d_value

        @pl.when((z1 < z) & early)
        def _():
            pair_tile(z1)
        return 0

    lax.fori_loop(0, zs + 1, own_step, 0)

    @pl.when(early)
    def _():
        for r in range(1, np):
            later(r)

    @pl.when((z == 0) & (y == 1))
    def _():
        ship(zs, part[zs, 0], part[zs, 1])
        for r in range(np):
            pair_fin(r).start()

    @pl.when(z == 0)
    def _():
        dq_recv[...] = jnp.zeros_like(dq_recv)

    dq_own[...] = jnp.transpose(dqt[0])

    @pl.when(late)
    def _():
        swapped()

        def pair_step(z1, _):
            @pl.when(z1 < z)
            def _():
                pair_tile(z1)
            return 0

        lax.fori_loop(0, zs, pair_step, 0)
        for r in range(1, np):
            later(r)

    @pl.when(swapping)
    def _():
        @pl.when(y == 0)
        def _():
            with jax.named_scope("pair_own"):
                d_key, d_value = tile(1, own[0], own[1], me, False)
                acc[0] += d_key
                acc[1] += d_value

        pair_dq = jnp.transpose(dqt[1]).astype(BF16)
        for r in range(np):
            for g in range(group):
                dq_send[r, g] = pair_dq[g * cap + r * half:g * cap + (r + 1) * half]
            swap_dq(r).start()

    pltpu.make_async_copy(w.at[0], w.at[0], w_sem.at[0]).wait()
    remote(w.at[1], w.at[1], w_send.at[0], w_recv.at[0], heads=other).wait_recv()
    width = mine // ns

    def g_copy(r):
        return remote(gs.at[0, r], gs.at[1, r], g_send.at[0], g_recv.at[r], heads=other)

    def whole(dx, s, n, r):
        cols = slice(dx * mine + s * width, dx * mine + (s + n) * width)
        return dot(gs[0, r], w[0, cols, :], NT) + dot(gs[1, r], w[1, cols, :], NT)

    def cross_copy(dx, r, i):
        at = (dx - 1, r, pl.ds(*plan[r][i]))
        return remote(
            xsend.at[at], xrcv.at[at], x_send.at[0], x_recv.at[dx - 1, first[r] + i], heads=across[dx]
        )

    for r in range(np):
        rows = slice(r * half, (r + 1) * half)

        def collect(i, _):
            z2 = zs - i

            @pl.when(((z2 > z) & (z2 < zs)) | ((z2 == zs) & (z == 0) & (y == 0)))
            def _():
                fin_wait(r, z2)
                acc[:, rows, :] += frcv[z2, r].astype(F32)
            return 0

        with jax.named_scope("wait_dq"):
            @pl.when(swapping)
            def _():
                swap_dq(r).wait_recv()
        for g in range(group):
            total = dq_own[g * cap + r * half:g * cap + (r + 1) * half, :] + dq_recv[r, g].astype(F32)
            gs[0, r, :, g * dim:(g + 1) * dim] = (total * scale).astype(BF16)
        with jax.named_scope("collect"):
            lax.fori_loop(0, zs + 1, collect, 0)
        key_total = acc[0, rows, :] * scale
        value_total = acc[1, rows, :]
        dk_ref[rows, :] = key_total
        dv_ref[rows, :] = value_total
        gs[0, r, :, wide:wide + dim] = key_total.astype(BF16)
        gs[0, r, :, wide + dim:wide + 2 * dim] = value_total.astype(BF16)
        g_copy(r).start()
        with jax.named_scope("wait_g"):
            g_copy(r).wait_recv()
        with jax.named_scope("project"):
            for dx in range(1, nx):
                for i, (s, n) in enumerate(plan[r]):
                    terms = whole(dx, s, n, r).astype(BF16)
                    for j in range(n):
                        xsend[dx - 1, r, s + j] = terms[:, j * width:(j + 1) * width]
                    cross_copy(dx, r, i).start()
    with jax.named_scope("own_proj"):
        for r in range(np):
            for s in range(0, ns, 2):
                hold[r * half:(r + 1) * half, s * width:(s + 2) * width] = whole(0, s, 2, r)
    for r in range(np):
        rows = slice(r * half, (r + 1) * half)
        for i, (s, n) in enumerate(plan[r]):
            for dx in range(1, nx):
                with jax.named_scope("wait_cross"):
                    cross_copy(dx, r, i).wait_recv()
            for j in range(s, s + n):
                cols = slice(j * width, (j + 1) * width)
                total = hold[rows, cols]
                for dx in range(1, nx):
                    total = total + xrcv[dx - 1, r, j].astype(F32)
                out_ref[rows, cols] = total.astype(BF16)

    with jax.named_scope("drain"):
        pl.when(late)(swap_q.wait_send)

        @pl.when(swapping)
        def _():
            swap_do.wait_send()
            swap_stats.wait_send()
            remote(dq_send, dq_recv, swap_send.at[2], swap_recv.at[2], ctx=pair).wait_send()

        def fins_sent(z1):
            remote(fsend.at[z1], frcv.at[z1], f_send.at[z1], f_recv.at[z1, 0], ctx=pair).wait_send()

        def drain(z2, _):
            @pl.when(z2 > z)
            def _():
                own_copy(z2).wait_send()

            @pl.when(z2 < z)
            def _():
                fins_sent(z2)
            return 0

        lax.fori_loop(0, zs, drain, 0)

        @pl.when((z == 0) & (y == 0))
        def _():
            pair_own_copy.wait_send()

        @pl.when((z == 0) & (y == 1))
        def _():
            fins_sent(zs)

        remote(w.at[1], w.at[1], w_send.at[0], w_recv.at[0], heads=other).wait_send()
        remote(gs.at[0], gs.at[1], g_send.at[0], g_recv.at[0], heads=other).wait_send()
        for dx in range(1, nx):
            remote(
                xsend.at[dx - 1], xrcv.at[dx - 1], x_send.at[0], x_recv.at[dx - 1, 0], heads=across[dx]
            ).wait_send()


def emit(a, b, c, a_hbm, b_hbm, c_hbm, sem):
    copies = [
        pltpu.make_async_copy(src, dst, sem.at[i])
        for i, (src, dst) in enumerate(((a, a_hbm), (b, b_hbm), (c, c_hbm)))
    ]
    for copy in copies:
        copy.start()
    for copy in copies:
        copy.wait()


def on_device(
    n, nh, queries, key_states, value_states, attention_out, out_grad, log_sum_exp, block_counts,
    w_query, w_key, w_value,
):
    zs, nx, ns = n // 2, nh // 2, 4
    cap, dim = key_states.shape
    width = queries.shape[1]
    rows = width // dim * cap
    model = w_query.shape[0]
    mine = model // nh
    chunk = mine // ns
    vmem = pl.BlockSpec(memory_space=pltpu.VMEM)
    half = BLOCK
    np = cap // half
    blocks = sum(len(p) for p in row_blocks(np, ns))
    hbm = pl.BlockSpec(memory_space=pltpu.HBM)
    dma = pltpu.SemaphoreType.DMA
    results = pl.pallas_call(
        functools.partial(kernel, zs, nx, ns),
        out_shape=(
            jax.ShapeDtypeStruct((cap, mine), BF16),
            jax.ShapeDtypeStruct((cap, dim), F32),
            jax.ShapeDtypeStruct((cap, dim), F32),
        ),
        in_specs=[hbm] * 10,
        out_specs=(vmem, vmem, vmem),
        scratch_shapes=[
            pltpu.SMEM(block_counts.shape, jnp.int32),
            pltpu.VMEM((2, cap, dim), BF16),
            pltpu.VMEM((2, cap, width), BF16),
            pltpu.VMEM((cap, width), BF16),
            pltpu.VMEM(log_sum_exp.shape, F32),
            pltpu.VMEM((2, cap, width), BF16),
            pltpu.VMEM((2, nx * mine, width + 2 * dim), BF16),
            pltpu.VMEM((2, rows, dim), BF16),
            pltpu.VMEM((2, rows, dim), BF16),
            pltpu.VMEM((2, 2, rows), F32),
            pltpu.VMEM((2, dim, rows), F32),
            pltpu.VMEM((rows, dim), F32),
            pltpu.VMEM((np, width // dim, half, dim), BF16),
            pltpu.VMEM((np, width // dim, half, dim), BF16),
            pltpu.VMEM((2, np, half, width + 2 * dim), BF16),
            pltpu.VMEM((2, cap, dim), F32),
            pltpu.VMEM((zs + 1, 2, cap, dim), BF16),
            pltpu.VMEM((zs + 1, 2, cap, dim), F32),
            pltpu.VMEM((zs + 1, np, 2, half, dim), BF16),
            pltpu.VMEM((zs + 1, np, 2, half, dim), BF16),
            pltpu.VMEM((cap, mine), F32),
            pltpu.VMEM((nx - 1, np, ns, half, chunk), BF16),
            pltpu.VMEM((nx - 1, np, ns, half, chunk), BF16),
            dma((5,)),
            dma((1,)),
            dma((1,)),
            dma((1,)),
            dma((zs + 1,)),
            dma((zs + 1,)),
            dma((4,)),
            dma((3 + np,)),
            dma((zs + 1,)),
            dma((zs + 1, np)),
            dma((1,)),
            dma((np,)),
            dma((1,)),
            dma((nx - 1, blocks)),
            pltpu.SemaphoreType.REGULAR,
        ],
        compiler_params=pltpu.CompilerParams(
            collective_id=0, has_side_effects=True, vmem_limit_bytes=52 * 1024 * 1024
        ),
    )(
        *(
            pltpu.with_memory_space_constraint(a, pltpu.HBM)
            for a in (
                queries, key_states, value_states, attention_out, out_grad, log_sum_exp,
                block_counts, w_query, w_key, w_value,
            )
        )
    )
    return pl.pallas_call(
        emit,
        out_shape=tuple(jax.ShapeDtypeStruct(a.shape, a.dtype) for a in results),
        in_specs=[vmem] * 3,
        out_specs=(hbm,) * 3,
        scratch_shapes=[dma((3,))],
    )(*(pltpu.with_memory_space_constraint(a, pltpu.VMEM) for a in results))


def solution(mesh):
    return jax.shard_map(
        functools.partial(on_device, mesh.shape["ctx"], mesh.shape["heads"]),
        mesh=mesh,
        in_specs=(
            P("ctx", "heads"),
            P("ctx", "heads"),
            P("ctx", "heads"),
            P("ctx", "heads"),
            P("ctx", "heads"),
            P("heads", "ctx"),
            P(),
            P(None, "heads"),
            P(None, "heads"),
            P(None, "heads"),
        ),
        out_specs=(P("ctx", "heads"), P("ctx", "heads"), P("ctx", "heads")),
        check_vma=False,
    )
```

```python
import functools
import math

import jax
import jax.numpy as jnp
from jax import lax
from jax.experimental import pallas as pl
from jax.experimental.pallas import tpu as pltpu
from jax.sharding import PartitionSpec as P

BLOCK = 64
EMIT = 4
LOG2E = math.log2(math.e)
F32 = jnp.float32
BF16 = jnp.bfloat16
NT = (((1,), (1,)), ((), ()))
TN = (((0,), (0,)), ((), ()))


def dot(a, b, dims=(((1,), (0,)), ((), ()))):
    return lax.dot_general(a, b, dims, preferred_element_type=F32)


def row_blocks(np, ns):
    plan = []
    for r in range(np):
        if r == 0:
            plan.append(((0, 1), (1, 1), (2, ns - 2)))
        elif r == np - 1:
            plan.append(((0, ns - 2), (ns - 2, 1), (ns - 1, 1)))
        else:
            plan.append(((0, ns // 2), (ns // 2, ns - ns // 2)))
    return plan


def kernel(
    zs, nx, ns,
    q_hbm, k_hbm, v_hbm, o_hbm, do_hbm, lse_hbm, cnt_hbm, wq_hbm, wk_hbm, wv_hbm,
    out_ref, dk_ref, dv_ref,
    cnt_ref, own, qd, o_ref, lse_ref, w, stats, dqt,
    dq_own, dq_send, dq_recv, gs, acc, kv, part, fsend, frcv, keep, hold, xsend, xrcv,
    in_sem, w_sem, w_send, w_recv, own_send, kv_recv, swap_send, swap_recv, f_send, f_recv,
    g_send, g_recv, x_send, x_recv, turn,
):
    cap, dim = own.shape[1:]
    group = qd.shape[1]
    np = dq_send.shape[0]
    half = cap // np
    scale = 1.0 / math.sqrt(dim)
    plan = row_blocks(np, ns)
    first = [sum(len(p) for p in plan[:r]) for r in range(np)]
    me = lax.axis_index("ctx")
    y = lax.rem(me, 2)
    z = lax.div(me, 2)
    pair = me + 1 - 2 * y
    h = lax.axis_index("heads")
    core = lax.rem(h, 2)
    x = lax.div(h, 2)
    other = h + 1 - 2 * core
    across = [2 * lax.rem(x + dx, nx) + core for dx in range(nx)]

    def remote(src, dst, send, recv, **device):
        return pltpu.make_async_remote_copy(
            src_ref=src, dst_ref=dst, send_sem=send, recv_sem=recv,
            device_id=device, device_id_type=pl.DeviceIdType.MESH,
        )

    mine = w.shape[1] // nx
    wide = group * dim
    weights = ((wq_hbm, 0, wide), (wk_hbm, wide, dim), (wv_hbm, wide + dim, dim))

    def w_rows(owner, src):
        return src.at[pl.ds(pl.multiple_of(owner * mine, mine), mine), :]

    w_loads = [
        pltpu.make_async_copy(
            w_rows(across[dx], src), w.at[0, pl.ds(dx * mine, mine), pl.ds(at, size)], w_sem.at[0]
        )
        for dx in range(nx)
        for src, at, size in weights
    ]
    w_shares = [
        remote(
            w_rows(across[dx] + 1 - 2 * core, src), w.at[1, pl.ds(dx * mine, mine), pl.ds(at, size)],
            w_send.at[0], w_recv.at[0], heads=other,
        )
        for dx in range(nx)
        for src, at, size in weights
    ]
    barrier = pltpu.get_barrier_semaphore()

    def greet(**device):
        pl.semaphore_signal(
            barrier, inc=1, device_id=device, device_id_type=pl.DeviceIdType.MESH
        )

    def greet_line(z2, _):
        @pl.when(z2 != z)
        def _():
            greet(ctx=2 * z2 + y)
        return 0

    lax.fori_loop(0, zs, greet_line, 0)
    greet(ctx=pair)
    greet(heads=other)
    for dx in range(1, nx):
        greet(heads=across[dx])

    heads = [pl.ds(g * dim, dim) for g in range(group)]
    loads = [
        pltpu.make_async_copy(src, dst, in_sem.at[i])
        for src, dst, i in (
            (k_hbm, own.at[0], 0), (v_hbm, own.at[1], 0),
            *((q_hbm.at[:, heads[g]], qd.at[0, g, 0], 1) for g in range(group)),
            *((do_hbm.at[:, heads[g]], qd.at[0, g, 1], 1) for g in range(group)),
            *((o_hbm.at[:, heads[g]], o_ref.at[g], 2) for g in range(group)),
            (lse_hbm, lse_ref, 3), (cnt_hbm, cnt_ref, 4),
        )
    ]
    for copy in loads:
        copy.start()
    pltpu.make_async_copy(own, own, in_sem.at[0]).wait()
    pltpu.make_async_copy(qd.at[0], qd.at[0], in_sem.at[1]).wait()
    pltpu.make_async_copy(o_ref, o_ref, in_sem.at[2]).wait()
    for copy in loads[-2:]:
        copy.wait()
    for copy in w_loads:
        copy.start()
    with jax.named_scope("barrier"):
        pl.semaphore_wait(barrier, zs + nx)

    def own_copy(z2):
        return remote(own, kv.at[z], own_send.at[z2], kv_recv.at[z], ctx=2 * z2 + y)

    pair_own_copy = remote(own, kv.at[zs], own_send.at[zs], kv_recv.at[zs], ctx=pair)

    def arrived(z1):
        remote(kv.at[z1], kv.at[z1], own_send.at[z1], kv_recv.at[z1], ctx=pair).wait_recv()

    swap_qd = [
        remote(qd.at[0, g], qd.at[1, g], swap_send.at[g], swap_recv.at[g], ctx=pair)
        for g in range(group)
    ]
    swap_stats = remote(
        stats.at[0], stats.at[1], swap_send.at[group], swap_recv.at[group], ctx=pair
    )

    def swap_dq(r):
        return remote(
            dq_send.at[r], dq_recv.at[r], swap_send.at[group + 1], swap_recv.at[group + 1 + r], ctx=pair
        )

    def fin_copy(r, z1):
        return remote(
            fsend.at[z1, r], frcv.at[z, r], f_send.at[z1], f_recv.at[z, r], ctx=2 * z1 + y
        )

    def pair_fin(r):
        return remote(
            fsend.at[zs, r], frcv.at[zs, r], f_send.at[zs], f_recv.at[zs, r], ctx=pair
        )

    def fin_wait(r, z2):
        remote(
            fsend.at[z2, r], frcv.at[z2, r], f_send.at[z2], f_recv.at[z2, r], ctx=pair
        ).wait_recv()

    swapping = z > 0
    early = swapping & (core == 0)
    late = swapping & (core == 1)

    @pl.when(early)
    def _():
        for copy in swap_qd:
            copy.start()

    @pl.when((z == 0) & (y == 0))
    def _():
        pair_own_copy.start()

    def push_own(i, _):
        z2 = zs - 1 - i

        @pl.when(z2 > z)
        def _():
            own_copy(z2).start()
        return 0

    lax.fori_loop(0, zs, push_own, 0)

    lane = lax.broadcasted_iota(jnp.int32, (1, group * cap), 1)
    row = lax.rem(lane, cap)
    alive = row < cnt_ref[me] * BLOCK
    def flat(ref):
        return ref[...].reshape(group * cap, dim)

    prod = flat(qd.at[0, :, 1]).astype(F32) * flat(o_ref).astype(F32)
    stats[0, 1:2] = lax.dot_general(
        jnp.ones((8, dim), F32), prod, NT,
        preferred_element_type=F32, precision=lax.Precision.HIGHEST,
    )[0:1]
    lse_row = jnp.concatenate([lse_ref[g:g + 1, :] for g in range(group)], axis=1)
    stats[0, 0:1] = jnp.where(alive, lse_row * LOG2E, 1e30)

    @pl.when(swapping)
    def _():
        swap_stats.start()

    key_row = lax.broadcasted_iota(jnp.int32, (cap, group * cap), 0)

    def products(key, value, query, out_grad, lse, delta, visible):
        scores = dot(key, query, NT)
        prob_grad = dot(value, out_grad, NT)
        prob = jnp.where(visible, jnp.exp2(scores * (scale * LOG2E) - lse), 0.0)
        grad = (prob * (prob_grad - delta)).astype(BF16)
        return dot(grad, query), dot(prob.astype(BF16), out_grad), dot(key, grad, TN)

    def tile(who, key, value, b, diagonal):
        visible = key_row < cnt_ref[b] * BLOCK
        if diagonal:
            visible = visible & (key_row <= row)
        d_key, d_value, terms = products(
            key, value, flat(qd.at[who, :, 0]), flat(qd.at[who, :, 1]),
            stats[who, 0:1], stats[who, 1:2], visible,
        )
        if diagonal:
            dqt[who] = terms
        else:
            dqt[who] += terms
        return d_key, d_value

    with jax.named_scope("diag"):
        d_key, d_value = tile(0, own[0], own[1], me, True)
        acc[0] = d_key
        acc[1] = d_value

    for copy in w_shares:
        copy.start()

    @pl.when(early)
    def _():
        with jax.named_scope("hand_over"):
            for copy in swap_qd[:group // 2]:
                copy.wait_send()
            pl.semaphore_signal(
                turn, inc=1, device_id={"heads": other}, device_id_type=pl.DeviceIdType.MESH
            )

    @pl.when(late)
    def _():
        with jax.named_scope("my_turn"):
            pl.semaphore_wait(turn, 1)
            for copy in swap_qd:
                copy.start()

    def ship(z1, d_key, d_value, pieces):
        for r in pieces:
            fsend[z1, r, 0] = d_key[r * half:(r + 1) * half].astype(BF16)
            fsend[z1, r, 1] = d_value[r * half:(r + 1) * half].astype(BF16)

    def later(r):
        def step(z1, _):
            sent = ((z1 == 0) & (early | (z > 1))) if r == 1 else z1 < 0

            @pl.when((z1 < z) & jnp.logical_not(sent))
            def _():
                fin_copy(r, z1).start()
            return 0
        lax.fori_loop(0, zs, step, 0)

    def last_pieces():
        for r in range(2, np):
            later(r)

    def swapped():
        dqt[1] = jnp.zeros_like(dqt[1])
        with jax.named_scope("wait_swap"):
            swap_stats.wait_recv()
            for copy in swap_qd:
                copy.wait_recv()

    def leave(z1, d_key, d_value):
        ship(z1, d_key, d_value, range(1))
        fin_copy(0, z1).start()
        ship(z1, d_key, d_value, range(1, np))

    def pair_tile(z1):
        with jax.named_scope("pair_tile"):
            d_key, d_value = tile(1, kv[z1, 0], kv[z1, 1], 2 * z1 + y, False)
            leave(z1, part[z1, 0] + d_key, part[z1, 1] + d_value)

        @pl.when(((z1 == 0) & early) | ((z1 == 1) & late))
        def _():
            fin_copy(1, 0).start()

    def own_step(z1, _):
        @pl.when((z1 < z) | ((z1 == zs) & (z == 0) & (y == 1)))
        def _():
            with jax.named_scope("wait_kv"):
                arrived(z1)
            with jax.named_scope("own_tile"):
                b = jnp.where(z1 == zs, pair, 2 * z1 + y)
                d_key, d_value = tile(0, kv[z1, 0], kv[z1, 1], b, False)
                part[z1, 0] = d_key
                part[z1, 1] = d_value

        pl.when((z1 == 0) & early)(swapped)

        @pl.when((z1 < z) & early)
        def _():
            pair_tile(z1)
        return 0

    lax.fori_loop(0, zs + 1, own_step, 0)

    @pl.when(early)
    def _():
        later(1)
        pl.when(z == zs - 1)(last_pieces)

    @pl.when((z == 0) & (y == 1))
    def _():
        ship(zs, part[zs, 0], part[zs, 1], range(np))
        for r in range(np):
            pair_fin(r).start()

    @pl.when(z == 0)
    def _():
        dq_recv[...] = jnp.zeros_like(dq_recv)

    dq_own[...] = jnp.transpose(dqt[0])

    @pl.when(late)
    def _():
        swapped()

        def pair_step(z1, _):
            @pl.when(z1 < z)
            def _():
                pair_tile(z1)
            return 0

        lax.fori_loop(0, zs, pair_step, 0)
        later(1)
        pl.when(z == zs - 1)(last_pieces)

    @pl.when(swapping & (y == 0))
    def _():
        with jax.named_scope("pair_own"):
            d_key, d_value = tile(1, own[0], own[1], me, False)
            acc[0] += d_key
            acc[1] += d_value

    @pl.when(swapping)
    def _():
        pair_dq = jnp.transpose(dqt[1]).astype(BF16)
        for r in range(np):
            for g in range(group):
                dq_send[r, g] = pair_dq[g * cap + r * half:g * cap + (r + 1) * half]
            swap_dq(r).start()

    pltpu.make_async_copy(w.at[0], w.at[0], w_sem.at[0]).wait()
    remote(w.at[1], w.at[1], w_send.at[0], w_recv.at[0], heads=other).wait_recv()
    width = mine // ns

    def g_copy(r):
        return remote(gs.at[0, r], gs.at[1, r], g_send.at[0], g_recv.at[r], heads=other)

    def side(c, dx, s, n, r):
        cols = slice(dx * mine + s * width, dx * mine + (s + n) * width)
        return dot(gs[c, r], w[c, cols, :], NT)

    def whole(dx, s, n, r):
        return side(0, dx, s, n, r) + side(1, dx, s, n, r)

    def cross_copy(dx, r, i):
        at = (dx - 1, r, pl.ds(*plan[r][i]))
        return remote(
            xsend.at[at], xrcv.at[at], x_send.at[0], x_recv.at[dx - 1, first[r] + i], heads=across[dx]
        )

    for r in range(np):
        rows = slice(r * half, (r + 1) * half)

        def collect(i, _):
            z2 = lax.rem(i + zs, zs + 1)

            @pl.when(((z2 > z) & (z2 < zs)) | ((z2 == zs) & (z == 0) & (y == 0)))
            def _():
                fin_wait(r, z2)
                acc[:, rows, :] += frcv[z2, r].astype(F32)
            return 0

        with jax.named_scope("wait_dq"):
            @pl.when(swapping)
            def _():
                swap_dq(r).wait_recv()
        if r == 0:
            pl.when(z < zs - 1)(last_pieces)
        for g in range(group):
            total = dq_own[g * cap + r * half:g * cap + (r + 1) * half, :] + dq_recv[r, g].astype(F32)
            gs[0, r, :, g * dim:(g + 1) * dim] = (total * scale).astype(BF16)
        with jax.named_scope("collect"):
            lax.fori_loop(0, zs + 1, collect, 0)
        key_total = acc[0, rows, :] * scale
        value_total = acc[1, rows, :]
        gs[0, r, :, wide:wide + dim] = key_total.astype(BF16)
        gs[0, r, :, wide + dim:wide + 2 * dim] = value_total.astype(BF16)
        g_copy(r).start()
        dk_ref[rows, :] = key_total
        dv_ref[rows, :] = value_total
        blocks = [(dx, i) for dx in range(1, nx) for i in range(len(plan[r]))]

        def half_sum(dx, i):
            s, n = plan[r][i]
            keep[dx - 1, :, s * width:(s + n) * width] = side(0, dx, s, n, r)

        def finish(dx, i):
            s, n = plan[r][i]
            terms = keep[dx - 1, :, s * width:(s + n) * width] + side(1, dx, s, n, r)
            terms = terms.astype(BF16)
            for j in range(n):
                xsend[dx - 1, r, s + j] = terms[:, j * width:(j + 1) * width]
            cross_copy(dx, r, i).start()

        def waiting():
            with jax.named_scope("half"):
                for dx, i in blocks:
                    half_sum(dx, i)
            with jax.named_scope("wait_g"):
                g_copy(r).wait_recv()
            with jax.named_scope("project"):
                for dx, i in blocks:
                    finish(dx, i)

        def ready():
            with jax.named_scope("wait_g"):
                g_copy(r).wait_recv()
            with jax.named_scope("project"):
                for dx, i in blocks:
                    half_sum(dx, i)
                    finish(dx, i)

        if r == 0:
            pl.when(core == 0)(waiting)
            pl.when(core == 1)(ready)
        else:
            waiting()
    with jax.named_scope("own_proj"):
        for r in range(np):
            for s in range(0, ns, 2):
                hold[r * half:(r + 1) * half, s * width:(s + 2) * width] = whole(0, s, 2, r)
    for r in range(np):
        rows = slice(r * half, (r + 1) * half)
        for i, (s, n) in enumerate(plan[r]):
            for dx in range(1, nx):
                with jax.named_scope("wait_cross"):
                    cross_copy(dx, r, i).wait_recv()
            for j in range(s, s + n):
                cols = slice(j * width, (j + 1) * width)
                total = hold[rows, cols]
                for dx in range(1, nx):
                    total = total + xrcv[dx - 1, r, j].astype(F32)
                out_ref[rows, cols] = total.astype(BF16)

    with jax.named_scope("drain"):
        @pl.when(late)
        def _():
            for copy in swap_qd[:group // 2]:
                copy.wait_send()

        @pl.when(swapping)
        def _():
            for copy in swap_qd[group // 2:]:
                copy.wait_send()
            swap_stats.wait_send()
            remote(dq_send, dq_recv, swap_send.at[group + 1], swap_recv.at[group + 1], ctx=pair).wait_send()

        def fins_sent(z1):
            remote(fsend.at[z1], frcv.at[z1], f_send.at[z1], f_recv.at[z1, 0], ctx=pair).wait_send()

        def drain(z2, _):
            @pl.when(z2 > z)
            def _():
                own_copy(z2).wait_send()

            @pl.when(z2 < z)
            def _():
                fins_sent(z2)
            return 0

        lax.fori_loop(0, zs, drain, 0)

        @pl.when((z == 0) & (y == 0))
        def _():
            pair_own_copy.wait_send()

        @pl.when((z == 0) & (y == 1))
        def _():
            fins_sent(zs)

        remote(w.at[1], w.at[1], w_send.at[0], w_recv.at[0], heads=other).wait_send()
        remote(gs.at[0], gs.at[1], g_send.at[0], g_recv.at[0], heads=other).wait_send()
        for dx in range(1, nx):
            remote(
                xsend.at[dx - 1], xrcv.at[dx - 1], x_send.at[0], x_recv.at[dx - 1, 0], heads=across[dx]
            ).wait_send()


def emit(parts, *refs):
    sem = refs[-1]
    copies = []
    for src, dst, n in zip(refs, refs[len(parts):], parts):
        step = src.shape[0] // n
        for i in range(n):
            at = pl.ds(i * step, step)
            copies.append(pltpu.make_async_copy(src.at[at], dst.at[at], sem.at[len(copies)]))
    for copy in copies:
        copy.start()
    for copy in copies:
        copy.wait()


def on_device(
    n, nh, queries, key_states, value_states, attention_out, out_grad, log_sum_exp, block_counts,
    w_query, w_key, w_value,
):
    zs, nx, ns = n // 2, nh // 2, 4
    cap, dim = key_states.shape
    width = queries.shape[1]
    rows = width // dim * cap
    model = w_query.shape[0]
    mine = model // nh
    chunk = mine // ns
    vmem = pl.BlockSpec(memory_space=pltpu.VMEM)
    half = BLOCK
    np = cap // half
    blocks = sum(len(p) for p in row_blocks(np, ns))
    hbm = pl.BlockSpec(memory_space=pltpu.HBM)
    dma = pltpu.SemaphoreType.DMA
    results = pl.pallas_call(
        functools.partial(kernel, zs, nx, ns),
        out_shape=(
            jax.ShapeDtypeStruct((cap, mine), BF16),
            jax.ShapeDtypeStruct((cap, dim), F32),
            jax.ShapeDtypeStruct((cap, dim), F32),
        ),
        in_specs=[hbm] * 10,
        out_specs=(vmem, vmem, vmem),
        scratch_shapes=[
            pltpu.SMEM(block_counts.shape, jnp.int32),
            pltpu.VMEM((2, cap, dim), BF16),
            pltpu.VMEM((2, width // dim, 2, cap, dim), BF16),
            pltpu.VMEM((width // dim, cap, dim), BF16),
            pltpu.VMEM(log_sum_exp.shape, F32),
            pltpu.VMEM((2, nx * mine, width + 2 * dim), BF16),
            pltpu.VMEM((2, 2, rows), F32),
            pltpu.VMEM((2, dim, rows), F32),
            pltpu.VMEM((rows, dim), F32),
            pltpu.VMEM((np, width // dim, half, dim), BF16),
            pltpu.VMEM((np, width // dim, half, dim), BF16),
            pltpu.VMEM((2, np, half, width + 2 * dim), BF16),
            pltpu.VMEM((2, cap, dim), F32),
            pltpu.VMEM((zs + 1, 2, cap, dim), BF16),
            pltpu.VMEM((zs + 1, 2, cap, dim), F32),
            pltpu.VMEM((zs + 1, np, 2, half, dim), BF16),
            pltpu.VMEM((zs + 1, np, 2, half, dim), BF16),
            pltpu.VMEM((nx - 1, half, mine), F32),
            pltpu.VMEM((cap, mine), F32),
            pltpu.VMEM((nx - 1, np, ns, half, chunk), BF16),
            pltpu.VMEM((nx - 1, np, ns, half, chunk), BF16),
            dma((5,)),
            dma((1,)),
            dma((1,)),
            dma((1,)),
            dma((zs + 1,)),
            dma((zs + 1,)),
            dma((width // dim + 2,)),
            dma((width // dim + 1 + np,)),
            dma((zs + 1,)),
            dma((zs + 1, np)),
            dma((1,)),
            dma((np,)),
            dma((1,)),
            dma((nx - 1, blocks)),
            pltpu.SemaphoreType.REGULAR,
        ],
        compiler_params=pltpu.CompilerParams(
            collective_id=0, has_side_effects=True, vmem_limit_bytes=52 * 1024 * 1024
        ),
    )(
        *(
            pltpu.with_memory_space_constraint(a, pltpu.HBM)
            for a in (
                queries, key_states, value_states, attention_out, out_grad, log_sum_exp,
                block_counts, w_query, w_key, w_value,
            )
        )
    )
    return pl.pallas_call(
        functools.partial(emit, (EMIT, 1, 1)),
        out_shape=tuple(jax.ShapeDtypeStruct(a.shape, a.dtype) for a in results),
        in_specs=[vmem] * 3,
        out_specs=(hbm,) * 3,
        scratch_shapes=[dma((EMIT + 2,))],
    )(*(pltpu.with_memory_space_constraint(a, pltpu.VMEM) for a in results))


def solution(mesh):
    return jax.shard_map(
        functools.partial(on_device, mesh.shape["ctx"], mesh.shape["heads"]),
        mesh=mesh,
        in_specs=(
            P("ctx", "heads"),
            P("ctx", "heads"),
            P("ctx", "heads"),
            P("ctx", "heads"),
            P("ctx", "heads"),
            P("heads", "ctx"),
            P(),
            P(None, "heads"),
            P(None, "heads"),
            P(None, "heads"),
        ),
        out_specs=(P("ctx", "heads"), P("ctx", "heads"), P("ctx", "heads")),
        check_vma=False,
    )
```

```python
import functools
import math

import jax
import jax.numpy as jnp
from jax import lax
from jax.experimental import pallas as pl
from jax.experimental.pallas import tpu as pltpu
from jax.sharding import PartitionSpec as P

BLOCK = 64
EMIT = 2
LOG2E = math.log2(math.e)
F32 = jnp.float32
BF16 = jnp.bfloat16
NT = (((1,), (1,)), ((), ()))
TN = (((0,), (0,)), ((), ()))


def dot(a, b, dims=(((1,), (0,)), ((), ()))):
    return lax.dot_general(a, b, dims, preferred_element_type=F32)


def row_blocks(np, ns):
    plan = []
    for r in range(np):
        if r == 0:
            plan.append(((0, 1), (1, 1), (2, ns - 2)))
        elif r == np - 1:
            plan.append(((0, ns - 2), (ns - 2, 1), (ns - 1, 1)))
        else:
            plan.append(((0, ns // 2), (ns // 2, ns - ns // 2)))
    return plan


def body(
    zs, nx, ns,
    q_hbm, k_hbm, v_hbm, o_hbm, do_hbm, lse_hbm, cnt_hbm, wq_hbm, wk_hbm, wv_hbm,
    out_ref, dk_ref, dv_ref,
    cnt_ref, own, qd, o_ref, lse_ref, w, stats, dqt,
    dq_own, dq_send, dq_recv, gs, acc, kv, part, fsend, frcv, keep, hold, xsend, xrcv,
    w_recv, kv_recv, swap_recv, f_recv, g_recv, x_recv, turn,
    in_sem, w_sem, w_send, own_send, swap_send, f_send, g_send, x_send,
):
    cap, dim = own.shape[1:]
    group = qd.shape[1]
    np = dq_send.shape[0]
    half = cap // np
    scale = 1.0 / math.sqrt(dim)
    plan = row_blocks(np, ns)
    first = [sum(len(p) for p in plan[:r]) for r in range(np)]
    me = lax.axis_index("ctx")
    y = lax.rem(me, 2)
    z = lax.div(me, 2)
    pair = me + 1 - 2 * y
    h = lax.axis_index("heads")
    core = lax.rem(h, 2)
    x = lax.div(h, 2)
    other = h + 1 - 2 * core
    across = [h] + [2 * lax.rem(x + dx, nx) + 1 - core for dx in range(1, nx)]
    theirs = [other] + [2 * lax.rem(x + dx, nx) + core for dx in range(1, nx)]

    def remote(src, dst, send, recv, **device):
        return pltpu.make_async_remote_copy(
            src_ref=src, dst_ref=dst, send_sem=send, recv_sem=recv,
            device_id=device, device_id_type=pl.DeviceIdType.MESH,
        )

    mine = w.shape[1] // nx
    wide = group * dim
    weights = ((wq_hbm, 0, wide), (wk_hbm, wide, dim), (wv_hbm, wide + dim, dim))

    def w_rows(owner, src):
        return src.at[pl.ds(pl.multiple_of(owner * mine, mine), mine), :]

    w_loads = [
        pltpu.make_async_copy(
            w_rows(across[dx], src), w.at[0, pl.ds(dx * mine, mine), pl.ds(at, size)], w_sem.at[0]
        )
        for dx in range(nx)
        for src, at, size in weights
    ]
    w_shares = [
        remote(
            w_rows(theirs[dx], src), w.at[1, pl.ds(dx * mine, mine), pl.ds(at, size)],
            w_send.at[0], w_recv.at[0], heads=other,
        )
        for dx in range(nx)
        for src, at, size in weights
    ]
    barrier = pltpu.get_barrier_semaphore()

    def greet(**device):
        pl.semaphore_signal(
            barrier, inc=1, device_id=device, device_id_type=pl.DeviceIdType.MESH
        )

    def greet_line(z2, _):
        @pl.when(z2 != z)
        def _():
            greet(ctx=2 * z2 + y)
        return 0

    lax.fori_loop(0, zs, greet_line, 0)
    greet(ctx=pair)
    greet(heads=other)
    for dx in range(1, nx):
        greet(heads=across[dx])

    heads = [pl.ds(g * dim, dim) for g in range(group)]
    loads = [
        pltpu.make_async_copy(src, dst, in_sem.at[i])
        for src, dst, i in (
            (k_hbm, own.at[0], 0), (v_hbm, own.at[1], 0),
            *((q_hbm.at[:, heads[g]], qd.at[0, g, 0], 1) for g in range(group)),
            *((do_hbm.at[:, heads[g]], qd.at[0, g, 1], 1) for g in range(group)),
            *((o_hbm.at[:, heads[g]], o_ref.at[g], 2) for g in range(group)),
            (lse_hbm, lse_ref, 3), (cnt_hbm, cnt_ref, 4),
        )
    ]
    for copy in loads:
        copy.start()
    pltpu.make_async_copy(own, own, in_sem.at[0]).wait()
    pltpu.make_async_copy(qd.at[0], qd.at[0], in_sem.at[1]).wait()
    pltpu.make_async_copy(o_ref, o_ref, in_sem.at[2]).wait()
    for copy in loads[-2:]:
        copy.wait()
    for copy in w_loads:
        copy.start()
    with jax.named_scope("barrier"):
        pl.semaphore_wait(barrier, zs + nx)

    def own_copy(z2):
        return remote(own, kv.at[z], own_send.at[z2], kv_recv.at[z], ctx=2 * z2 + y)

    pair_own_copy = remote(own, kv.at[zs - 1], own_send.at[0], kv_recv.at[zs - 1], ctx=pair)

    def arrived(z1):
        remote(kv.at[z1], kv.at[z1], own_send.at[z1], kv_recv.at[z1], ctx=pair).wait_recv()

    swap_qd = [
        remote(qd.at[0, g], qd.at[1, g], swap_send.at[g], swap_recv.at[g], ctx=pair)
        for g in range(group)
    ]
    swap_stats = remote(
        stats.at[0], stats.at[1], swap_send.at[group], swap_recv.at[group], ctx=pair
    )

    def swap_dq(r):
        return remote(
            dq_send.at[r], dq_recv.at[r], swap_send.at[group + 1], swap_recv.at[group + 1 + r], ctx=pair
        )

    def fin_copy(r, z1):
        return remote(
            fsend.at[z1, r], frcv.at[z, r], f_send.at[z1], f_recv.at[z, r], ctx=2 * z1 + y
        )

    def pair_fin(r):
        return remote(
            fsend.at[zs - 1, r], frcv.at[0, r], f_send.at[zs - 1], f_recv.at[0, r], ctx=pair
        )

    def fin_wait(r, z2):
        remote(
            fsend.at[z2, r], frcv.at[z2, r], f_send.at[z2], f_recv.at[z2, r], ctx=pair
        ).wait_recv()

    swapping = z > 0
    early = swapping & (core == 0)
    late = swapping & (core == 1)

    @pl.when(early)
    def _():
        for copy in swap_qd:
            copy.start()

    @pl.when((z == 0) & (y == 0))
    def _():
        pair_own_copy.start()

    def push_own(i, _):
        z2 = zs - 1 - i

        @pl.when(z2 > z)
        def _():
            own_copy(z2).start()
        return 0

    lax.fori_loop(0, zs, push_own, 0)

    lane = lax.broadcasted_iota(jnp.int32, (1, group * cap), 1)
    row = lax.rem(lane, cap)
    alive = row < cnt_ref[me] * BLOCK
    def flat(ref):
        return ref[...].reshape(group * cap, dim)

    prod = flat(qd.at[0, :, 1]).astype(F32) * flat(o_ref).astype(F32)
    stats[0, 1:2] = lax.dot_general(
        jnp.ones((8, dim), F32), prod, NT,
        preferred_element_type=F32, precision=lax.Precision.HIGHEST,
    )[0:1]
    lse_row = jnp.concatenate([lse_ref[g:g + 1, :] for g in range(group)], axis=1)
    stats[0, 0:1] = jnp.where(alive, lse_row * LOG2E, 1e30)

    @pl.when(swapping)
    def _():
        swap_stats.start()

    key_row = lax.broadcasted_iota(jnp.int32, (cap, group * cap), 0)

    def products(key, value, query, out_grad, lse, delta, visible):
        scores = dot(key, query, NT)
        prob_grad = dot(value, out_grad, NT)
        prob = jnp.where(visible, jnp.exp2(scores * (scale * LOG2E) - lse), 0.0)
        grad = (prob * (prob_grad - delta)).astype(BF16)
        return dot(grad, query), dot(prob.astype(BF16), out_grad), dot(key, grad, TN)

    def tile(who, key, value, b, diagonal):
        visible = key_row < cnt_ref[b] * BLOCK
        if diagonal:
            visible = visible & (key_row <= row)
        d_key, d_value, terms = products(
            key, value, flat(qd.at[who, :, 0]), flat(qd.at[who, :, 1]),
            stats[who, 0:1], stats[who, 1:2], visible,
        )
        if diagonal:
            dqt[who] = terms
        else:
            dqt[who] += terms
        return d_key, d_value

    with jax.named_scope("diag"):
        d_key, d_value = tile(0, own[0], own[1], me, True)
        acc[0] = d_key
        acc[1] = d_value

    for copy in w_shares:
        copy.start()

    @pl.when(early)
    def _():
        with jax.named_scope("hand_over"):
            for copy in swap_qd[:group // 2]:
                copy.wait_send()
            pl.semaphore_signal(
                turn, inc=1, device_id={"heads": other}, device_id_type=pl.DeviceIdType.MESH
            )

    @pl.when(late)
    def _():
        with jax.named_scope("my_turn"):
            pl.semaphore_wait(turn, 1)
            for copy in swap_qd:
                copy.start()

    def ship(z1, d_key, d_value, pieces):
        for r in pieces:
            fsend[z1, r, 0] = d_key[r * half:(r + 1) * half].astype(BF16)
            fsend[z1, r, 1] = d_value[r * half:(r + 1) * half].astype(BF16)

    def later(r):
        def step(z1, _):
            sent = ((z1 == 0) & (early | (z > 1))) if r == 1 else z1 < 0

            @pl.when((z1 < z) & jnp.logical_not(sent))
            def _():
                fin_copy(r, z1).start()
            return 0
        lax.fori_loop(0, zs, step, 0)

    def last_pieces():
        for r in range(2, np):
            later(r)

    def swapped():
        dqt[1] = jnp.zeros_like(dqt[1])
        with jax.named_scope("wait_swap"):
            swap_stats.wait_recv()
            for copy in swap_qd:
                copy.wait_recv()

    def leave(z1, d_key, d_value):
        ship(z1, d_key, d_value, range(1))
        fin_copy(0, z1).start()
        ship(z1, d_key, d_value, range(1, np))

    def pair_tile(z1):
        with jax.named_scope("pair_tile"):
            d_key, d_value = tile(1, kv[z1, 0], kv[z1, 1], 2 * z1 + y, False)
            leave(z1, part[z1, 0] + d_key, part[z1, 1] + d_value)

        @pl.when(((z1 == 0) & early) | ((z1 == 1) & late))
        def _():
            fin_copy(1, 0).start()

    def own_step(z1, _):
        @pl.when((z1 < z) | ((z1 == zs - 1) & (z == 0) & (y == 1)))
        def _():
            with jax.named_scope("wait_kv"):
                arrived(z1)
            with jax.named_scope("own_tile"):
                b = jnp.where(z == 0, pair, 2 * z1 + y)
                d_key, d_value = tile(0, kv[z1, 0], kv[z1, 1], b, False)
                part[z1, 0] = d_key
                part[z1, 1] = d_value

        pl.when((z1 == 0) & early)(swapped)

        @pl.when((z1 < z) & early)
        def _():
            pair_tile(z1)
        return 0

    lax.fori_loop(0, zs, own_step, 0)

    @pl.when(early)
    def _():
        later(1)
        pl.when(z == zs - 1)(last_pieces)

    @pl.when((z == 0) & (y == 1))
    def _():
        ship(zs - 1, part[zs - 1, 0], part[zs - 1, 1], range(np))
        for r in range(np):
            pair_fin(r).start()

    @pl.when(z == 0)
    def _():
        dq_recv[...] = jnp.zeros_like(dq_recv)

    dq_own[...] = jnp.transpose(dqt[0])

    @pl.when(late)
    def _():
        swapped()

        def pair_step(z1, _):
            @pl.when(z1 < z)
            def _():
                pair_tile(z1)
            return 0

        lax.fori_loop(0, zs, pair_step, 0)
        later(1)
        pl.when(z == zs - 1)(last_pieces)

    @pl.when(swapping & (y == 0))
    def _():
        with jax.named_scope("pair_own"):
            d_key, d_value = tile(1, own[0], own[1], me, False)
            acc[0] += d_key
            acc[1] += d_value

    @pl.when(swapping)
    def _():
        pair_dq = jnp.transpose(dqt[1]).astype(BF16)
        for r in range(np):
            for g in range(group):
                dq_send[r, g] = pair_dq[g * cap + r * half:g * cap + (r + 1) * half]
            swap_dq(r).start()

    pltpu.make_async_copy(w.at[0], w.at[0], w_sem.at[0]).wait()
    remote(w.at[1], w.at[1], w_send.at[0], w_recv.at[0], heads=other).wait_recv()
    width = mine // ns

    def g_copy(r, at=0, size=None):
        columns = pl.ds(at, wide + 2 * dim if size is None else size)
        return remote(
            gs.at[0, r, :, columns], gs.at[1, r, :, columns], g_send.at[0], g_recv.at[r], heads=other
        )

    def side(c, dx, s, n, r):
        cols = slice(dx * mine + s * width, dx * mine + (s + n) * width)
        return dot(gs[c, r], w[c, cols, :], NT)

    def whole(dx, s, n, r):
        return side(0, dx, s, n, r) + side(1, dx, s, n, r)

    def cross_copy(dx, r, i):
        at = (dx - 1, r, pl.ds(*plan[r][i]))
        return remote(
            xsend.at[at], xrcv.at[at], x_send.at[0], x_recv.at[dx - 1, first[r] + i], heads=across[dx]
        )

    for r in range(np):
        rows = slice(r * half, (r + 1) * half)

        def collect(z2, _):
            @pl.when((z2 > z) | ((z2 == 0) & (z == 0) & (y == 0)))
            def _():
                fin_wait(r, z2)
                acc[:, rows, :] += frcv[z2, r].astype(F32)
            return 0

        with jax.named_scope("wait_dq"):
            @pl.when(swapping)
            def _():
                swap_dq(r).wait_recv()
        if r == 0:
            pl.when(z < zs - 1)(last_pieces)
        for g in range(group):
            total = dq_own[g * cap + r * half:g * cap + (r + 1) * half, :] + dq_recv[r, g].astype(F32)
            gs[0, r, :, g * dim:(g + 1) * dim] = (total * scale).astype(BF16)
        g_copy(r, 0, wide).start()
        with jax.named_scope("collect"):
            lax.fori_loop(0, zs, collect, 0)
        key_total = acc[0, rows, :] * scale
        value_total = acc[1, rows, :]
        gs[0, r, :, wide:wide + dim] = key_total.astype(BF16)
        gs[0, r, :, wide + dim:wide + 2 * dim] = value_total.astype(BF16)
        g_copy(r, wide, 2 * dim).start()
        dk_ref[rows, :] = key_total
        dv_ref[rows, :] = value_total
        blocks = [(dx, i) for dx in range(1, nx) for i in range(len(plan[r]))]

        def half_sum(dx, i):
            s, n = plan[r][i]
            keep[dx - 1, :, s * width:(s + n) * width] = side(0, dx, s, n, r)

        def finish(dx, i):
            s, n = plan[r][i]
            terms = keep[dx - 1, :, s * width:(s + n) * width] + side(1, dx, s, n, r)
            terms = terms.astype(BF16)
            for j in range(n):
                xsend[dx - 1, r, s + j] = terms[:, j * width:(j + 1) * width]
            cross_copy(dx, r, i).start()

        def waiting():
            with jax.named_scope("half"):
                for dx, i in blocks:
                    half_sum(dx, i)
            with jax.named_scope("wait_g"):
                g_copy(r).wait_recv()
            with jax.named_scope("project"):
                for dx, i in blocks:
                    finish(dx, i)

        def ready():
            with jax.named_scope("wait_g"):
                g_copy(r).wait_recv()
            with jax.named_scope("project"):
                for dx, i in blocks:
                    half_sum(dx, i)
                    finish(dx, i)

        if r == 0:
            pl.when(core == 0)(waiting)
            pl.when(core == 1)(ready)
        else:
            waiting()
    with jax.named_scope("own_proj"):
        for r in range(np):
            for s in range(0, ns, 2):
                hold[r * half:(r + 1) * half, s * width:(s + 2) * width] = whole(0, s, 2, r)
    for r in range(np):
        rows = slice(r * half, (r + 1) * half)
        for i, (s, n) in enumerate(plan[r]):
            for dx in range(1, nx):
                with jax.named_scope("wait_cross"):
                    cross_copy(dx, r, i).wait_recv()
            for j in range(s, s + n):
                cols = slice(j * width, (j + 1) * width)
                total = hold[rows, cols]
                for dx in range(1, nx):
                    total = total + xrcv[dx - 1, r, j].astype(F32)
                out_ref[rows, cols] = total.astype(BF16)

    with jax.named_scope("drain"):
        @pl.when(late)
        def _():
            for copy in swap_qd[:group // 2]:
                copy.wait_send()

        @pl.when(swapping)
        def _():
            for copy in swap_qd[group // 2:]:
                copy.wait_send()
            swap_stats.wait_send()
            remote(dq_send, dq_recv, swap_send.at[group + 1], swap_recv.at[group + 1], ctx=pair).wait_send()

        def fins_sent(z1):
            remote(fsend.at[z1], frcv.at[z1], f_send.at[z1], f_recv.at[z1, 0], ctx=pair).wait_send()

        def drain(z2, _):
            @pl.when(z2 > z)
            def _():
                own_copy(z2).wait_send()

            @pl.when(z2 < z)
            def _():
                fins_sent(z2)
            return 0

        lax.fori_loop(0, zs, drain, 0)

        @pl.when((z == 0) & (y == 0))
        def _():
            pair_own_copy.wait_send()

        @pl.when((z == 0) & (y == 1))
        def _():
            fins_sent(zs - 1)

        remote(w.at[1], w.at[1], w_send.at[0], w_recv.at[0], heads=other).wait_send()
        remote(gs.at[0], gs.at[1], g_send.at[0], g_recv.at[0], heads=other).wait_send()
        for dx in range(1, nx):
            remote(
                xsend.at[dx - 1], xrcv.at[dx - 1], x_send.at[0], x_recv.at[dx - 1, 0], heads=across[dx]
            ).wait_send()


def kernel(zs, nx, ns, group, *refs):
    dma = pltpu.SemaphoreType.DMA
    pl.run_scoped(
        functools.partial(body, zs, nx, ns, *refs),
        in_sem=dma((5,)), w_sem=dma((1,)), w_send=dma((1,)), own_send=dma((zs,)),
        swap_send=dma((group + 2,)), f_send=dma((zs,)), g_send=dma((1,)), x_send=dma((1,)),
    )


def emit(parts, *refs):
    sem = refs[-1]
    copies = []
    for src, dst, n in zip(refs, refs[len(parts):], parts):
        step = src.shape[0] // n
        for i in range(n):
            at = pl.ds(i * step, step)
            copies.append(pltpu.make_async_copy(src.at[at], dst.at[at], sem.at[len(copies)]))
    for copy in copies:
        copy.start()
    for copy in copies:
        copy.wait()


def on_device(
    n, nh, queries, key_states, value_states, attention_out, out_grad, log_sum_exp, block_counts,
    w_query, w_key, w_value,
):
    zs, nx, ns = n // 2, nh // 2, 4
    cap, dim = key_states.shape
    width = queries.shape[1]
    rows = width // dim * cap
    model = w_query.shape[0]
    mine = model // nh
    chunk = mine // ns
    vmem = pl.BlockSpec(memory_space=pltpu.VMEM)
    half = BLOCK
    np = cap // half
    blocks = sum(len(p) for p in row_blocks(np, ns))
    hbm = pl.BlockSpec(memory_space=pltpu.HBM)
    dma = pltpu.SemaphoreType.DMA
    results = pl.pallas_call(
        functools.partial(kernel, zs, nx, ns, width // dim),
        out_shape=(
            jax.ShapeDtypeStruct((cap, mine), BF16),
            jax.ShapeDtypeStruct((cap, dim), F32),
            jax.ShapeDtypeStruct((cap, dim), F32),
        ),
        in_specs=[hbm] * 10,
        out_specs=(vmem, vmem, vmem),
        scratch_shapes=[
            pltpu.SMEM(block_counts.shape, jnp.int32),
            pltpu.VMEM((2, cap, dim), BF16),
            pltpu.VMEM((2, width // dim, 2, cap, dim), BF16),
            pltpu.VMEM((width // dim, cap, dim), BF16),
            pltpu.VMEM(log_sum_exp.shape, F32),
            pltpu.VMEM((2, nx * mine, width + 2 * dim), BF16),
            pltpu.VMEM((2, 2, rows), F32),
            pltpu.VMEM((2, dim, rows), F32),
            pltpu.VMEM((rows, dim), F32),
            pltpu.VMEM((np, width // dim, half, dim), BF16),
            pltpu.VMEM((np, width // dim, half, dim), BF16),
            pltpu.VMEM((2, np, half, width + 2 * dim), BF16),
            pltpu.VMEM((2, cap, dim), F32),
            pltpu.VMEM((zs, 2, cap, dim), BF16),
            pltpu.VMEM((zs, 2, cap, dim), F32),
            pltpu.VMEM((zs, np, 2, half, dim), BF16),
            pltpu.VMEM((zs, np, 2, half, dim), BF16),
            pltpu.VMEM((nx - 1, half, mine), F32),
            pltpu.VMEM((cap, mine), F32),
            pltpu.VMEM((nx - 1, np, ns, half, chunk), BF16),
            pltpu.VMEM((nx - 1, np, ns, half, chunk), BF16),
            dma((1,)),
            dma((zs,)),
            dma((width // dim + 1 + np,)),
            dma((zs, np)),
            dma((np,)),
            dma((nx - 1, blocks)),
            pltpu.SemaphoreType.REGULAR,
        ],
        compiler_params=pltpu.CompilerParams(
            collective_id=0, has_side_effects=True, vmem_limit_bytes=52 * 1024 * 1024
        ),
    )(
        *(
            pltpu.with_memory_space_constraint(a, pltpu.HBM)
            for a in (
                queries, key_states, value_states, attention_out, out_grad, log_sum_exp,
                block_counts, w_query, w_key, w_value,
            )
        )
    )
    return pl.pallas_call(
        functools.partial(emit, (EMIT, 1, 1)),
        out_shape=tuple(jax.ShapeDtypeStruct(a.shape, a.dtype) for a in results),
        in_specs=[vmem] * 3,
        out_specs=(hbm,) * 3,
        scratch_shapes=[dma((EMIT + 2,))],
    )(*(pltpu.with_memory_space_constraint(a, pltpu.VMEM) for a in results))


def solution(mesh):
    return jax.shard_map(
        functools.partial(on_device, mesh.shape["ctx"], mesh.shape["heads"]),
        mesh=mesh,
        in_specs=(
            P("ctx", "heads"),
            P("ctx", "heads"),
            P("ctx", "heads"),
            P("ctx", "heads"),
            P("ctx", "heads"),
            P("heads", "ctx"),
            P(),
            P(None, "heads"),
            P(None, "heads"),
            P(None, "heads"),
        ),
        out_specs=(P("ctx", "heads"), P("ctx", "heads"), P("ctx", "heads")),
        check_vma=False,
    )
```

```python
import functools
import math

import jax
import jax.numpy as jnp
from jax import lax
from jax.experimental import pallas as pl
from jax.experimental.pallas import tpu as pltpu
from jax.sharding import PartitionSpec as P

BLOCK = 64
EMIT = 2
LOG2E = math.log2(math.e)
F32 = jnp.float32
BF16 = jnp.bfloat16
NT = (((1,), (1,)), ((), ()))
TN = (((0,), (0,)), ((), ()))


def dot(a, b, dims=(((1,), (0,)), ((), ()))):
    return lax.dot_general(a, b, dims, preferred_element_type=F32)


def row_blocks(np, ns):
    plan = []
    for r in range(np):
        if r == 0:
            plan.append(((0, 1), (1, 1), (2, ns - 2)))
        elif r == np - 1:
            plan.append(((0, ns - 2), (ns - 2, 1), (ns - 1, 1)))
        else:
            plan.append(((0, ns // 2), (ns // 2, ns - ns // 2)))
    return plan


def body(
    zs, nx, ns,
    q_hbm, k_hbm, v_hbm, o_hbm, do_hbm, lse_hbm, cnt_hbm, wq_hbm, wk_hbm, wv_hbm,
    out_ref, dk_ref, dv_ref,
    cnt_ref, own, qd, o_ref, lse_ref, w, wt, stats, dqt,
    dq_own, dq_send, dq_recv, gs, acc, kv, part, fsend, frcv, keep, hold, xsend, xrcv,
    w_recv, kv_recv, swap_recv, f_recv, g_recv, x_recv, turn,
    in_sem, w_sem, w_send, own_send, swap_send, f_send, g_send, x_send,
):
    cap, dim = own.shape[1:]
    group = qd.shape[1]
    np = dq_send.shape[0]
    half = cap // np
    scale = 1.0 / math.sqrt(dim)
    plan = row_blocks(np, ns)
    first = [sum(len(p) for p in plan[:r]) for r in range(np)]
    me = lax.axis_index("ctx")
    y = lax.rem(me, 2)
    z = lax.div(me, 2)
    pair = me + 1 - 2 * y
    h = lax.axis_index("heads")
    core = lax.rem(h, 2)
    x = lax.div(h, 2)
    other = h + 1 - 2 * core
    across = [h] + [2 * lax.rem(x + dx, nx) + 1 - core for dx in range(1, nx)]
    theirs = [other] + [2 * lax.rem(x + dx, nx) + core for dx in range(1, nx)]

    def remote(src, dst, send, recv, **device):
        return pltpu.make_async_remote_copy(
            src_ref=src, dst_ref=dst, send_sem=send, recv_sem=recv,
            device_id=device, device_id_type=pl.DeviceIdType.MESH,
        )

    mine = w.shape[1] // nx
    wide = group * dim
    weights = ((wq_hbm, 0, wide), (wk_hbm, wide, dim), (wv_hbm, wide + dim, dim))

    def w_rows(owner, src):
        return src.at[pl.ds(pl.multiple_of(owner * mine, mine), mine), :]

    w_loads = [
        pltpu.make_async_copy(
            w_rows(across[dx], src), w.at[0, pl.ds(dx * mine, mine), pl.ds(at, size)], w_sem.at[0]
        )
        for dx in range(nx)
        for src, at, size in weights
    ]
    w_shares = [
        remote(
            w_rows(theirs[dx], src), w.at[1, pl.ds(dx * mine, mine), pl.ds(at, size)],
            w_send.at[0], w_recv.at[0], heads=other,
        )
        for dx in range(nx)
        for src, at, size in weights
    ]
    barrier = pltpu.get_barrier_semaphore()

    def greet(**device):
        pl.semaphore_signal(
            barrier, inc=1, device_id=device, device_id_type=pl.DeviceIdType.MESH
        )

    def greet_line(z2, _):
        @pl.when(z2 != z)
        def _():
            greet(ctx=2 * z2 + y)
        return 0

    lax.fori_loop(0, zs, greet_line, 0)
    greet(ctx=pair)
    greet(heads=other)
    for dx in range(1, nx):
        greet(heads=across[dx])

    heads = [pl.ds(g * dim, dim) for g in range(group)]
    loads = [
        pltpu.make_async_copy(src, dst, in_sem.at[i])
        for src, dst, i in (
            (k_hbm, own.at[0], 0), (v_hbm, own.at[1], 0),
            *((q_hbm.at[:, heads[g]], qd.at[0, g, 0], 1) for g in range(group)),
            *((do_hbm.at[:, heads[g]], qd.at[0, g, 1], 1) for g in range(group)),
            *((o_hbm.at[:, heads[g]], o_ref.at[g], 2) for g in range(group)),
            (lse_hbm, lse_ref, 3), (cnt_hbm, cnt_ref, 4),
        )
    ]
    for copy in loads:
        copy.start()
    pltpu.make_async_copy(own, own, in_sem.at[0]).wait()
    pltpu.make_async_copy(qd.at[0], qd.at[0], in_sem.at[1]).wait()
    pltpu.make_async_copy(o_ref, o_ref, in_sem.at[2]).wait()
    for copy in loads[-2:]:
        copy.wait()
    for copy in w_loads:
        copy.start()
    with jax.named_scope("barrier"):
        pl.semaphore_wait(barrier, zs + nx)

    def own_copy(z2):
        return remote(own, kv.at[z], own_send.at[z2], kv_recv.at[z], ctx=2 * z2 + y)

    pair_own_copy = remote(own, kv.at[zs - 1], own_send.at[0], kv_recv.at[zs - 1], ctx=pair)

    def arrived(z1):
        remote(kv.at[z1], kv.at[z1], own_send.at[z1], kv_recv.at[z1], ctx=pair).wait_recv()

    swap_qd = [
        remote(qd.at[0, g], qd.at[1, g], swap_send.at[g], swap_recv.at[g], ctx=pair)
        for g in range(group)
    ]
    swap_stats = remote(
        stats.at[0], stats.at[1], swap_send.at[group], swap_recv.at[group], ctx=pair
    )

    def swap_dq(r):
        return remote(
            dq_send.at[r], dq_recv.at[r], swap_send.at[group + 1], swap_recv.at[group + 1 + r], ctx=pair
        )

    def fin_copy(r, z1):
        return remote(
            fsend.at[z1, r], frcv.at[z, r], f_send.at[z1], f_recv.at[z, r], ctx=2 * z1 + y
        )

    def pair_fin(r):
        return remote(
            fsend.at[zs - 1, r], frcv.at[0, r], f_send.at[zs - 1], f_recv.at[0, r], ctx=pair
        )

    def fin_wait(r, z2):
        remote(
            fsend.at[z2, r], frcv.at[z2, r], f_send.at[z2], f_recv.at[z2, r], ctx=pair
        ).wait_recv()

    swapping = z > 0
    early = swapping & (core == 0)
    late = swapping & (core == 1)

    @pl.when(early)
    def _():
        for copy in swap_qd:
            copy.start()

    @pl.when((z == 0) & (y == 0))
    def _():
        pair_own_copy.start()

    def push_own(i, _):
        z2 = zs - 1 - i

        @pl.when(z2 > z)
        def _():
            own_copy(z2).start()
        return 0

    lax.fori_loop(0, zs, push_own, 0)

    lane = lax.broadcasted_iota(jnp.int32, (1, group * cap), 1)
    row = lax.rem(lane, cap)
    alive = row < cnt_ref[me] * BLOCK
    def flat(ref):
        return ref[...].reshape(group * cap, dim)

    prod = flat(qd.at[0, :, 1]).astype(F32) * flat(o_ref).astype(F32)
    stats[0, 1:2] = lax.dot_general(
        jnp.ones((8, dim), F32), prod, NT,
        preferred_element_type=F32, precision=lax.Precision.HIGHEST,
    )[0:1]
    lse_row = jnp.concatenate([lse_ref[g:g + 1, :] for g in range(group)], axis=1)
    stats[0, 0:1] = jnp.where(alive, lse_row * LOG2E, 1e30)

    @pl.when(swapping)
    def _():
        swap_stats.start()

    key_row = lax.broadcasted_iota(jnp.int32, (cap, group * cap), 0)

    def products(key, value, query, out_grad, lse, delta, visible):
        scores = dot(key, query, NT)
        prob_grad = dot(value, out_grad, NT)
        prob = jnp.where(visible, jnp.exp2(scores * (scale * LOG2E) - lse), 0.0)
        grad = (prob * (prob_grad - delta)).astype(BF16)
        return dot(grad, query), dot(prob.astype(BF16), out_grad), dot(key, grad, TN)

    def tile(who, key, value, b, diagonal):
        visible = key_row < cnt_ref[b] * BLOCK
        if diagonal:
            visible = visible & (key_row <= row)
        d_key, d_value, terms = products(
            key, value, flat(qd.at[who, :, 0]), flat(qd.at[who, :, 1]),
            stats[who, 0:1], stats[who, 1:2], visible,
        )
        if diagonal:
            dqt[who] = terms
        else:
            dqt[who] += terms
        return d_key, d_value

    with jax.named_scope("diag"):
        d_key, d_value = tile(0, own[0], own[1], me, True)
        acc[0] = d_key
        acc[1] = d_value

    for copy in w_shares:
        copy.start()

    @pl.when(early)
    def _():
        with jax.named_scope("hand_over"):
            for copy in swap_qd[:group // 2]:
                copy.wait_send()
            pl.semaphore_signal(
                turn, inc=1, device_id={"heads": other}, device_id_type=pl.DeviceIdType.MESH
            )

    @pl.when(late)
    def _():
        with jax.named_scope("my_turn"):
            pl.semaphore_wait(turn, 1)
            for copy in swap_qd:
                copy.start()

    def turn_w(c):
        def step(i, _):
            at = pl.ds(pl.multiple_of(i * 256, 256), 256)
            wt[c, :, at] = jnp.transpose(w[c, at, :])
            return 0
        with jax.named_scope("turn_w"):
            lax.fori_loop(0, w.shape[1] // 256, step, 0)

    pltpu.make_async_copy(w.at[0], w.at[0], w_sem.at[0]).wait()
    turn_w(0)

    def ship(z1, d_key, d_value, pieces):
        for r in pieces:
            fsend[z1, r, 0] = d_key[r * half:(r + 1) * half].astype(BF16)
            fsend[z1, r, 1] = d_value[r * half:(r + 1) * half].astype(BF16)

    def later(pieces):
        def step(z1, _):
            for r in pieces:
                sent = ((z1 == 0) & (early | (z > 1))) if r < np - 1 else z1 < 0

                @pl.when((z1 < z) & jnp.logical_not(sent))
                def _():
                    fin_copy(r, z1).start()
            return 0
        lax.fori_loop(0, zs, step, 0)

    def last_pieces():
        later([np - 1])

    def swapped():
        dqt[1] = jnp.zeros_like(dqt[1])
        with jax.named_scope("wait_swap"):
            swap_stats.wait_recv()
            for copy in swap_qd:
                copy.wait_recv()

    def leave(z1, d_key, d_value):
        ship(z1, d_key, d_value, range(1))
        fin_copy(0, z1).start()
        ship(z1, d_key, d_value, range(1, np))

    def pair_tile(z1):
        with jax.named_scope("pair_tile"):
            d_key, d_value = tile(1, kv[z1, 0], kv[z1, 1], 2 * z1 + y, False)
            leave(z1, part[z1, 0] + d_key, part[z1, 1] + d_value)

        @pl.when(((z1 == 0) & early) | ((z1 == 1) & late))
        def _():
            for r in range(1, np - 1):
                fin_copy(r, 0).start()

    def own_step(z1, _):
        @pl.when((z1 < z) | ((z1 == zs - 1) & (z == 0) & (y == 1)))
        def _():
            with jax.named_scope("wait_kv"):
                arrived(z1)
            with jax.named_scope("own_tile"):
                b = jnp.where(z == 0, pair, 2 * z1 + y)
                d_key, d_value = tile(0, kv[z1, 0], kv[z1, 1], b, False)
                part[z1, 0] = d_key
                part[z1, 1] = d_value

        pl.when((z1 == 0) & early)(swapped)

        @pl.when((z1 < z) & early)
        def _():
            pair_tile(z1)
        return 0

    lax.fori_loop(0, zs, own_step, 0)

    @pl.when(early)
    def _():
        later(range(1, np - 1))
        pl.when(z == zs - 1)(last_pieces)

    @pl.when((z == 0) & (y == 1))
    def _():
        ship(zs - 1, part[zs - 1, 0], part[zs - 1, 1], range(np))
        for r in range(np):
            pair_fin(r).start()

    @pl.when(z == 0)
    def _():
        dq_recv[...] = jnp.zeros_like(dq_recv)

    dq_own[...] = jnp.transpose(dqt[0])

    @pl.when(late)
    def _():
        swapped()

        def pair_step(z1, _):
            @pl.when(z1 < z)
            def _():
                pair_tile(z1)
            return 0

        lax.fori_loop(0, zs, pair_step, 0)
        later(range(1, np - 1))
        pl.when(z == zs - 1)(last_pieces)

    @pl.when(swapping & (y == 0))
    def _():
        with jax.named_scope("pair_own"):
            d_key, d_value = tile(1, own[0], own[1], me, False)
            acc[0] += d_key
            acc[1] += d_value

    @pl.when(swapping)
    def _():
        pair_dq = jnp.transpose(dqt[1]).astype(BF16)
        for r in range(np):
            for g in range(group):
                dq_send[r, g] = pair_dq[g * cap + r * half:g * cap + (r + 1) * half]
            swap_dq(r).start()

    width = mine // ns

    def g_copy(r, at=0, size=None):
        columns = pl.ds(at, wide + 2 * dim if size is None else size)
        return remote(
            gs.at[0, r, :, columns], gs.at[1, r, :, columns], g_send.at[0], g_recv.at[r], heads=other
        )

    def side(c, dx, s, n, r):
        cols = slice(dx * mine + s * width, dx * mine + (s + n) * width)
        return dot(gs[c, r], wt[c, :, cols])

    def whole(dx, s, n, r):
        return side(0, dx, s, n, r) + side(1, dx, s, n, r)

    def cross_copy(dx, r, i):
        at = (dx - 1, r, pl.ds(*plan[r][i]))
        return remote(
            xsend.at[at], xrcv.at[at], x_send.at[0], x_recv.at[dx - 1, first[r] + i], heads=across[dx]
        )

    remote(w.at[1], w.at[1], w_send.at[0], w_recv.at[0], heads=other).wait_recv()
    turn_w(1)

    for r in range(np):
        rows = slice(r * half, (r + 1) * half)

        def collect(z2, _):
            @pl.when((z2 > z) | ((z2 == 0) & (z == 0) & (y == 0)))
            def _():
                fin_wait(r, z2)
                acc[:, rows, :] += frcv[z2, r].astype(F32)
            return 0

        with jax.named_scope("wait_dq"):
            @pl.when(swapping)
            def _():
                swap_dq(r).wait_recv()
        if r == 0:
            pl.when(z < zs - 1)(last_pieces)
        for g in range(group):
            total = dq_own[g * cap + r * half:g * cap + (r + 1) * half, :] + dq_recv[r, g].astype(F32)
            gs[0, r, :, g * dim:(g + 1) * dim] = (total * scale).astype(BF16)
        g_copy(r, 0, wide).start()
        with jax.named_scope("collect"):
            lax.fori_loop(0, zs, collect, 0)
        key_total = acc[0, rows, :] * scale
        value_total = acc[1, rows, :]
        gs[0, r, :, wide:wide + dim] = key_total.astype(BF16)
        gs[0, r, :, wide + dim:wide + 2 * dim] = value_total.astype(BF16)
        g_copy(r, wide, 2 * dim).start()
        dk_ref[rows, :] = key_total
        dv_ref[rows, :] = value_total
        blocks = [(dx, i) for dx in range(1, nx) for i in range(len(plan[r]))]

        def half_sum(dx, i):
            s, n = plan[r][i]
            keep[dx - 1, :, s * width:(s + n) * width] = side(0, dx, s, n, r)

        def finish(dx, i):
            s, n = plan[r][i]
            terms = keep[dx - 1, :, s * width:(s + n) * width] + side(1, dx, s, n, r)
            terms = terms.astype(BF16)
            for j in range(n):
                xsend[dx - 1, r, s + j] = terms[:, j * width:(j + 1) * width]
            cross_copy(dx, r, i).start()

        def waiting():
            with jax.named_scope("half"):
                for dx, i in blocks:
                    half_sum(dx, i)
            with jax.named_scope("wait_g"):
                g_copy(r).wait_recv()
            with jax.named_scope("project"):
                for dx, i in blocks:
                    finish(dx, i)

        def ready():
            with jax.named_scope("wait_g"):
                g_copy(r).wait_recv()
            with jax.named_scope("project"):
                for dx, i in blocks:
                    half_sum(dx, i)
                    finish(dx, i)

        if r == 0:
            pl.when(core == 0)(waiting)
            pl.when(core == 1)(ready)
        else:
            waiting()
    with jax.named_scope("own_proj"):
        for r in range(np):
            for s in range(0, ns, 2):
                hold[r * half:(r + 1) * half, s * width:(s + 2) * width] = whole(0, s, 2, r)
    for r in range(np):
        rows = slice(r * half, (r + 1) * half)
        for i, (s, n) in enumerate(plan[r]):
            for dx in range(1, nx):
                with jax.named_scope("wait_cross"):
                    cross_copy(dx, r, i).wait_recv()
            for j in range(s, s + n):
                cols = slice(j * width, (j + 1) * width)
                total = hold[rows, cols]
                for dx in range(1, nx):
                    total = total + xrcv[dx - 1, r, j].astype(F32)
                out_ref[rows, cols] = total.astype(BF16)

    with jax.named_scope("drain"):
        @pl.when(late)
        def _():
            for copy in swap_qd[:group // 2]:
                copy.wait_send()

        @pl.when(swapping)
        def _():
            for copy in swap_qd[group // 2:]:
                copy.wait_send()
            swap_stats.wait_send()
            remote(dq_send, dq_recv, swap_send.at[group + 1], swap_recv.at[group + 1], ctx=pair).wait_send()

        def fins_sent(z1):
            remote(fsend.at[z1], frcv.at[z1], f_send.at[z1], f_recv.at[z1, 0], ctx=pair).wait_send()

        def drain(z2, _):
            @pl.when(z2 > z)
            def _():
                own_copy(z2).wait_send()

            @pl.when(z2 < z)
            def _():
                fins_sent(z2)
            return 0

        lax.fori_loop(0, zs, drain, 0)

        @pl.when((z == 0) & (y == 0))
        def _():
            pair_own_copy.wait_send()

        @pl.when((z == 0) & (y == 1))
        def _():
            fins_sent(zs - 1)

        remote(w.at[1], w.at[1], w_send.at[0], w_recv.at[0], heads=other).wait_send()
        remote(gs.at[0], gs.at[1], g_send.at[0], g_recv.at[0], heads=other).wait_send()
        for dx in range(1, nx):
            remote(
                xsend.at[dx - 1], xrcv.at[dx - 1], x_send.at[0], x_recv.at[dx - 1, 0], heads=across[dx]
            ).wait_send()


def kernel(zs, nx, ns, group, *refs):
    dma = pltpu.SemaphoreType.DMA
    pl.run_scoped(
        functools.partial(body, zs, nx, ns, *refs),
        in_sem=dma((5,)), w_sem=dma((1,)), w_send=dma((1,)), own_send=dma((zs,)),
        swap_send=dma((group + 2,)), f_send=dma((zs,)), g_send=dma((1,)), x_send=dma((1,)),
    )


def emit(parts, *refs):
    sem = refs[-1]
    copies = []
    for src, dst, n in zip(refs, refs[len(parts):], parts):
        step = src.shape[0] // n
        for i in range(n):
            at = pl.ds(i * step, step)
            copies.append(pltpu.make_async_copy(src.at[at], dst.at[at], sem.at[len(copies)]))
    for copy in copies:
        copy.start()
    for copy in copies:
        copy.wait()


def on_device(
    n, nh, queries, key_states, value_states, attention_out, out_grad, log_sum_exp, block_counts,
    w_query, w_key, w_value,
):
    zs, nx, ns = n // 2, nh // 2, 4
    cap, dim = key_states.shape
    width = queries.shape[1]
    rows = width // dim * cap
    model = w_query.shape[0]
    mine = model // nh
    chunk = mine // ns
    vmem = pl.BlockSpec(memory_space=pltpu.VMEM)
    half = cap // 4
    np = cap // half
    blocks = sum(len(p) for p in row_blocks(np, ns))
    hbm = pl.BlockSpec(memory_space=pltpu.HBM)
    dma = pltpu.SemaphoreType.DMA
    results = pl.pallas_call(
        functools.partial(kernel, zs, nx, ns, width // dim),
        out_shape=(
            jax.ShapeDtypeStruct((cap, mine), BF16),
            jax.ShapeDtypeStruct((cap, dim), F32),
            jax.ShapeDtypeStruct((cap, dim), F32),
        ),
        in_specs=[hbm] * 10,
        out_specs=(vmem, vmem, vmem),
        scratch_shapes=[
            pltpu.SMEM(block_counts.shape, jnp.int32),
            pltpu.VMEM((2, cap, dim), BF16),
            pltpu.VMEM((2, width // dim, 2, cap, dim), BF16),
            pltpu.VMEM((width // dim, cap, dim), BF16),
            pltpu.VMEM(log_sum_exp.shape, F32),
            pltpu.VMEM((2, nx * mine, width + 2 * dim), BF16),
            pltpu.VMEM((2, width + 2 * dim, nx * mine), BF16),
            pltpu.VMEM((2, 2, rows), F32),
            pltpu.VMEM((2, dim, rows), F32),
            pltpu.VMEM((rows, dim), F32),
            pltpu.VMEM((np, width // dim, half, dim), BF16),
            pltpu.VMEM((np, width // dim, half, dim), BF16),
            pltpu.VMEM((2, np, half, width + 2 * dim), BF16),
            pltpu.VMEM((2, cap, dim), F32),
            pltpu.VMEM((zs, 2, cap, dim), BF16),
            pltpu.VMEM((zs, 2, cap, dim), F32),
            pltpu.VMEM((zs, np, 2, half, dim), BF16),
            pltpu.VMEM((zs, np, 2, half, dim), BF16),
            pltpu.VMEM((nx - 1, half, mine), F32),
            pltpu.VMEM((cap, mine), F32),
            pltpu.VMEM((nx - 1, np, ns, half, chunk), BF16),
            pltpu.VMEM((nx - 1, np, ns, half, chunk), BF16),
            dma((1,)),
            dma((zs,)),
            dma((width // dim + 1 + np,)),
            dma((zs, np)),
            dma((np,)),
            dma((nx - 1, blocks)),
            pltpu.SemaphoreType.REGULAR,
        ],
        compiler_params=pltpu.CompilerParams(
            collective_id=0, has_side_effects=True, vmem_limit_bytes=52 * 1024 * 1024
        ),
    )(
        *(
            pltpu.with_memory_space_constraint(a, pltpu.HBM)
            for a in (
                queries, key_states, value_states, attention_out, out_grad, log_sum_exp,
                block_counts, w_query, w_key, w_value,
            )
        )
    )
    return pl.pallas_call(
        functools.partial(emit, (EMIT, 1, 1)),
        out_shape=tuple(jax.ShapeDtypeStruct(a.shape, a.dtype) for a in results),
        in_specs=[vmem] * 3,
        out_specs=(hbm,) * 3,
        scratch_shapes=[dma((EMIT + 2,))],
    )(*(pltpu.with_memory_space_constraint(a, pltpu.VMEM) for a in results))


def solution(mesh):
    return jax.shard_map(
        functools.partial(on_device, mesh.shape["ctx"], mesh.shape["heads"]),
        mesh=mesh,
        in_specs=(
            P("ctx", "heads"),
            P("ctx", "heads"),
            P("ctx", "heads"),
            P("ctx", "heads"),
            P("ctx", "heads"),
            P("heads", "ctx"),
            P(),
            P(None, "heads"),
            P(None, "heads"),
            P(None, "heads"),
        ),
        out_specs=(P("ctx", "heads"), P("ctx", "heads"), P("ctx", "heads")),
        check_vma=False,
    )
```

```python
import functools
import math

import jax
import jax.numpy as jnp
from jax import lax
from jax.experimental import pallas as pl
from jax.experimental.pallas import tpu as pltpu
from jax.sharding import PartitionSpec as P

BLOCK = 64
EMIT = 2
LOG2E = math.log2(math.e)
F32 = jnp.float32
BF16 = jnp.bfloat16
NT = (((1,), (1,)), ((), ()))
TN = (((0,), (0,)), ((), ()))


def dot(a, b, dims=(((1,), (0,)), ((), ()))):
    return lax.dot_general(a, b, dims, preferred_element_type=F32)


def row_blocks(np, ns):
    plan = []
    for r in range(np):
        if r == 0:
            plan.append(((0, 1), (1, 1), (2, ns - 2)))
        elif r == np - 1:
            plan.append(((0, ns - 2), (ns - 2, 1), (ns - 1, 1)))
        else:
            plan.append(((0, ns // 2), (ns // 2, ns - ns // 2)))
    return plan


def body(
    zs, nx, ns,
    q_hbm, k_hbm, v_hbm, o_hbm, do_hbm, lse_hbm, cnt_hbm, wq_hbm, wk_hbm, wv_hbm,
    out_ref, dk_ref, dv_ref,
    cnt_ref, own, qd, o_ref, lse_ref, w, wt, stats, dqt,
    dq_own, dq_send, dq_recv, gs, acc, kv, part, fsend, frcv, keep, hold, xsend, xrcv,
    w_recv, kv_recv, swap_recv, f_recv, g_recv, x_recv, turn,
    in_sem, w_sem, w_send, own_send, swap_send, f_send, g_send, x_send,
):
    cap, dim = own.shape[1:]
    group = qd.shape[1]
    np = dq_send.shape[0]
    half = cap // np
    scale = 1.0 / math.sqrt(dim)
    plan = row_blocks(np, ns)
    first = [sum(len(p) for p in plan[:r]) for r in range(np)]
    me = lax.axis_index("ctx")
    y = lax.rem(me, 2)
    z = lax.div(me, 2)
    pair = me + 1 - 2 * y
    h = lax.axis_index("heads")
    core = lax.rem(h, 2)
    x = lax.div(h, 2)
    other = h + 1 - 2 * core
    across = [h] + [2 * lax.rem(x + dx, nx) + 1 - core for dx in range(1, nx)]
    theirs = [other] + [2 * lax.rem(x + dx, nx) + core for dx in range(1, nx)]

    def remote(src, dst, send, recv, **device):
        return pltpu.make_async_remote_copy(
            src_ref=src, dst_ref=dst, send_sem=send, recv_sem=recv,
            device_id=device, device_id_type=pl.DeviceIdType.MESH,
        )

    mine = w.shape[1] // nx
    wide = group * dim
    weights = ((wq_hbm, 0, wide), (wk_hbm, wide, dim), (wv_hbm, wide + dim, dim))

    def w_rows(owner, src):
        return src.at[pl.ds(pl.multiple_of(owner * mine, mine), mine), :]

    w_loads = [
        pltpu.make_async_copy(
            w_rows(across[dx], src), w.at[0, pl.ds(dx * mine, mine), pl.ds(at, size)], w_sem.at[0]
        )
        for dx in range(nx)
        for src, at, size in weights
    ]
    w_shares = [
        remote(
            w_rows(theirs[dx], src), w.at[1, pl.ds(dx * mine, mine), pl.ds(at, size)],
            w_send.at[0], w_recv.at[0], heads=other,
        )
        for dx in range(nx)
        for src, at, size in weights
    ]
    barrier = pltpu.get_barrier_semaphore()

    def greet(**device):
        pl.semaphore_signal(
            barrier, inc=1, device_id=device, device_id_type=pl.DeviceIdType.MESH
        )

    def greet_line(z2, _):
        @pl.when(z2 != z)
        def _():
            greet(ctx=2 * z2 + y)
        return 0

    lax.fori_loop(0, zs, greet_line, 0)
    greet(ctx=pair)
    greet(heads=other)
    for dx in range(1, nx):
        greet(heads=across[dx])

    heads = [pl.ds(g * dim, dim) for g in range(group)]
    loads = [
        pltpu.make_async_copy(src, dst, in_sem.at[i])
        for src, dst, i in (
            (k_hbm, own.at[0], 0), (v_hbm, own.at[1], 0),
            *((q_hbm.at[:, heads[g]], qd.at[0, g, 0], 1) for g in range(group)),
            *((do_hbm.at[:, heads[g]], qd.at[0, g, 1], 1) for g in range(group)),
            *((o_hbm.at[:, heads[g]], o_ref.at[g], 2) for g in range(group)),
            (lse_hbm, lse_ref, 3), (cnt_hbm, cnt_ref, 4),
        )
    ]
    for copy in loads:
        copy.start()
    pltpu.make_async_copy(own, own, in_sem.at[0]).wait()
    pltpu.make_async_copy(qd.at[0], qd.at[0], in_sem.at[1]).wait()
    pltpu.make_async_copy(o_ref, o_ref, in_sem.at[2]).wait()
    for copy in loads[-2:]:
        copy.wait()
    for copy in w_loads:
        copy.start()
    with jax.named_scope("barrier"):
        pl.semaphore_wait(barrier, zs + nx)

    def own_copy(z2):
        return remote(own, kv.at[z], own_send.at[z2], kv_recv.at[z], ctx=2 * z2 + y)

    pair_own_copy = remote(own, kv.at[zs - 1], own_send.at[0], kv_recv.at[zs - 1], ctx=pair)

    def arrived(z1):
        remote(kv.at[z1], kv.at[z1], own_send.at[z1], kv_recv.at[z1], ctx=pair).wait_recv()

    swap_qd = [
        remote(qd.at[0, g], qd.at[1, g], swap_send.at[g], swap_recv.at[g], ctx=pair)
        for g in range(group)
    ]
    swap_stats = remote(
        stats.at[0], stats.at[1], swap_send.at[group], swap_recv.at[group], ctx=pair
    )

    def swap_dq(r):
        return remote(
            dq_send.at[r], dq_recv.at[r], swap_send.at[group + 1], swap_recv.at[group + 1 + r], ctx=pair
        )

    def fin_copy(r, z1):
        return remote(
            fsend.at[z1, r], frcv.at[z, r], f_send.at[z1], f_recv.at[z, r], ctx=2 * z1 + y
        )

    def pair_fin(r):
        return remote(
            fsend.at[zs - 1, r], frcv.at[0, r], f_send.at[zs - 1], f_recv.at[0, r], ctx=pair
        )

    def fin_wait(r, z2):
        remote(
            fsend.at[z2, r], frcv.at[z2, r], f_send.at[z2], f_recv.at[z2, r], ctx=pair
        ).wait_recv()

    swapping = z > 0
    early = swapping & (core == 0)
    late = swapping & (core == 1)

    @pl.when(early)
    def _():
        for copy in swap_qd:
            copy.start()

    @pl.when((z == 0) & (y == 0))
    def _():
        pair_own_copy.start()

    def push_own(i, _):
        z2 = zs - 1 - i

        @pl.when(z2 > z)
        def _():
            own_copy(z2).start()
        return 0

    lax.fori_loop(0, zs, push_own, 0)

    lane = lax.broadcasted_iota(jnp.int32, (1, group * cap), 1)
    row = lax.rem(lane, cap)
    alive = row < cnt_ref[me] * BLOCK
    def flat(ref):
        return ref[...].reshape(group * cap, dim)

    prod = flat(qd.at[0, :, 1]).astype(F32) * flat(o_ref).astype(F32)
    stats[0, 1:2] = lax.dot_general(
        jnp.ones((8, dim), F32), prod, NT,
        preferred_element_type=F32, precision=lax.Precision.HIGHEST,
    )[0:1]
    lse_row = jnp.concatenate([lse_ref[g:g + 1, :] for g in range(group)], axis=1)
    stats[0, 0:1] = jnp.where(alive, lse_row * LOG2E, 1e30)

    @pl.when(swapping)
    def _():
        swap_stats.start()

    key_row = lax.broadcasted_iota(jnp.int32, (cap, group * cap), 0)

    def products(key, value, query, out_grad, lse, delta, visible):
        scores = dot(key, query, NT)
        prob_grad = dot(value, out_grad, NT)
        prob = jnp.where(visible, jnp.exp2(scores * (scale * LOG2E) - lse), 0.0)
        grad = (prob * (prob_grad - delta)).astype(BF16)
        return dot(grad, query), dot(prob.astype(BF16), out_grad), dot(key, grad, TN)

    def tile(who, key, value, b, diagonal):
        visible = key_row < cnt_ref[b] * BLOCK
        if diagonal:
            visible = visible & (key_row <= row)
        d_key, d_value, terms = products(
            key, value, flat(qd.at[who, :, 0]), flat(qd.at[who, :, 1]),
            stats[who, 0:1], stats[who, 1:2], visible,
        )
        if diagonal:
            dqt[who] = terms
        else:
            dqt[who] += terms
        return d_key, d_value

    with jax.named_scope("diag"):
        d_key, d_value = tile(0, own[0], own[1], me, True)
        acc[0] = d_key
        acc[1] = d_value

    for copy in w_shares:
        copy.start()

    @pl.when(early)
    def _():
        with jax.named_scope("hand_over"):
            for copy in swap_qd[:3]:
                copy.wait_send()
            pl.semaphore_signal(
                turn, inc=1, device_id={"heads": other}, device_id_type=pl.DeviceIdType.MESH
            )

    @pl.when(late)
    def _():
        with jax.named_scope("my_turn"):
            pl.semaphore_wait(turn, 1)
            for copy in swap_qd:
                copy.start()

    def turn_w(c):
        def step(i, _):
            at = pl.ds(pl.multiple_of(i * 256, 256), 256)
            wt[c, :, at] = jnp.transpose(w[c, at, :])
            return 0
        with jax.named_scope("turn_w"):
            lax.fori_loop(0, w.shape[1] // 256, step, 0)

    pltpu.make_async_copy(w.at[0], w.at[0], w_sem.at[0]).wait()
    turn_w(0)

    def ship(z1, d_key, d_value, pieces):
        for r in pieces:
            fsend[z1, r, 0] = d_key[r * half:(r + 1) * half].astype(BF16)
            fsend[z1, r, 1] = d_value[r * half:(r + 1) * half].astype(BF16)

    def later(pieces):
        def step(z1, _):
            for r in pieces:
                sent = ((z1 == 0) & (early | ((z > 1) if r == 1 else False))) if r < np - 1 else z1 < 0

                @pl.when((z1 < z) & jnp.logical_not(sent))
                def _():
                    fin_copy(r, z1).start()
            return 0
        lax.fori_loop(0, zs, step, 0)

    def last_pieces():
        later([np - 1])

    def swapped():
        dqt[1] = jnp.zeros_like(dqt[1])
        with jax.named_scope("wait_swap"):
            swap_stats.wait_recv()
            for copy in swap_qd:
                copy.wait_recv()

    def leave(z1, d_key, d_value):
        ship(z1, d_key, d_value, range(1))
        fin_copy(0, z1).start()
        ship(z1, d_key, d_value, range(1, np))

    def pair_tile(z1):
        with jax.named_scope("pair_tile"):
            d_key, d_value = tile(1, kv[z1, 0], kv[z1, 1], 2 * z1 + y, False)
            leave(z1, part[z1, 0] + d_key, part[z1, 1] + d_value)

        @pl.when(((z1 == 0) & early) | ((z1 == 1) & late))
        def _():
            fin_copy(1, 0).start()

        @pl.when((z1 == 0) & early)
        def _():
            for r in range(2, np - 1):
                fin_copy(r, 0).start()

    def own_step(z1, _):
        @pl.when((z1 < z) | ((z1 == zs - 1) & (z == 0) & (y == 1)))
        def _():
            with jax.named_scope("wait_kv"):
                arrived(z1)
            with jax.named_scope("own_tile"):
                b = jnp.where(z == 0, pair, 2 * z1 + y)
                d_key, d_value = tile(0, kv[z1, 0], kv[z1, 1], b, False)
                part[z1, 0] = d_key
                part[z1, 1] = d_value

        pl.when((z1 == 0) & early)(swapped)

        @pl.when((z1 < z) & early)
        def _():
            pair_tile(z1)
        return 0

    lax.fori_loop(0, zs, own_step, 0)

    @pl.when(early)
    def _():
        later(range(1, np - 1))
        pl.when(z == zs - 1)(last_pieces)

    @pl.when((z == 0) & (y == 1))
    def _():
        ship(zs - 1, part[zs - 1, 0], part[zs - 1, 1], range(np))
        for r in range(np):
            pair_fin(r).start()

    @pl.when(z == 0)
    def _():
        dq_recv[...] = jnp.zeros_like(dq_recv)

    dq_own[...] = jnp.transpose(dqt[0])

    @pl.when(late)
    def _():
        swapped()

        def pair_step(z1, _):
            @pl.when(z1 < z)
            def _():
                pair_tile(z1)
            return 0

        lax.fori_loop(0, zs, pair_step, 0)
        later(range(1, np - 1))
        pl.when(z == zs - 1)(last_pieces)

    @pl.when(swapping & (y == 0))
    def _():
        with jax.named_scope("pair_own"):
            d_key, d_value = tile(1, own[0], own[1], me, False)
            acc[0] += d_key
            acc[1] += d_value

    @pl.when(swapping)
    def _():
        pair_dq = jnp.transpose(dqt[1]).astype(BF16)
        for r in range(np):
            for g in range(group):
                dq_send[r, g] = pair_dq[g * cap + r * half:g * cap + (r + 1) * half]
            swap_dq(r).start()

    width = mine // ns

    def g_copy(r, at=0, size=None):
        columns = pl.ds(at, wide + 2 * dim if size is None else size)
        return remote(
            gs.at[0, r, :, columns], gs.at[1, r, :, columns], g_send.at[0], g_recv.at[r], heads=other
        )

    def side(c, dx, s, n, r):
        cols = slice(dx * mine + s * width, dx * mine + (s + n) * width)
        return dot(gs[c, r], wt[c, :, cols])

    def whole(dx, s, n, r):
        return side(0, dx, s, n, r) + side(1, dx, s, n, r)

    def cross_copy(dx, r, i):
        at = (dx - 1, r, pl.ds(*plan[r][i]))
        return remote(
            xsend.at[at], xrcv.at[at], x_send.at[0], x_recv.at[dx - 1, first[r] + i], heads=across[dx]
        )

    remote(w.at[1], w.at[1], w_send.at[0], w_recv.at[0], heads=other).wait_recv()
    turn_w(1)

    for r in range(np):
        rows = slice(r * half, (r + 1) * half)

        def collect(z2, _):
            @pl.when((z2 > z) | ((z2 == 0) & (z == 0) & (y == 0)))
            def _():
                fin_wait(r, z2)
                acc[:, rows, :] += frcv[z2, r].astype(F32)
            return 0

        with jax.named_scope("wait_dq"):
            @pl.when(swapping)
            def _():
                swap_dq(r).wait_recv()
        if r == 0:
            pl.when(z < zs - 1)(last_pieces)
        for g in range(group):
            total = dq_own[g * cap + r * half:g * cap + (r + 1) * half, :] + dq_recv[r, g].astype(F32)
            gs[0, r, :, g * dim:(g + 1) * dim] = (total * scale).astype(BF16)
        g_copy(r, 0, wide).start()
        with jax.named_scope("collect"):
            lax.fori_loop(0, zs, collect, 0)
        key_total = acc[0, rows, :] * scale
        value_total = acc[1, rows, :]
        gs[0, r, :, wide:wide + dim] = key_total.astype(BF16)
        gs[0, r, :, wide + dim:wide + 2 * dim] = value_total.astype(BF16)
        g_copy(r, wide, 2 * dim).start()
        dk_ref[rows, :] = key_total
        dv_ref[rows, :] = value_total
        blocks = [(dx, i) for dx in range(1, nx) for i in range(len(plan[r]))]

        def half_sum(dx, i):
            s, n = plan[r][i]
            keep[dx - 1, :, s * width:(s + n) * width] = side(0, dx, s, n, r)

        def finish(dx, i):
            s, n = plan[r][i]
            terms = keep[dx - 1, :, s * width:(s + n) * width] + side(1, dx, s, n, r)
            terms = terms.astype(BF16)
            for j in range(n):
                xsend[dx - 1, r, s + j] = terms[:, j * width:(j + 1) * width]
            cross_copy(dx, r, i).start()

        def waiting():
            with jax.named_scope("half"):
                for dx, i in blocks:
                    half_sum(dx, i)
            with jax.named_scope("wait_g"):
                g_copy(r).wait_recv()
            with jax.named_scope("project"):
                for dx, i in blocks:
                    finish(dx, i)

        def ready():
            with jax.named_scope("wait_g"):
                g_copy(r).wait_recv()
            with jax.named_scope("project"):
                for dx, i in blocks:
                    half_sum(dx, i)
                    finish(dx, i)

        if r == 0:
            pl.when(core == 0)(waiting)
            pl.when(core == 1)(ready)
        else:
            waiting()
    with jax.named_scope("own_proj"):
        for r in range(np):
            for s in range(0, ns, 2):
                hold[r * half:(r + 1) * half, s * width:(s + 2) * width] = whole(0, s, 2, r)
    for r in range(np):
        rows = slice(r * half, (r + 1) * half)
        for i, (s, n) in enumerate(plan[r]):
            for dx in range(1, nx):
                with jax.named_scope("wait_cross"):
                    cross_copy(dx, r, i).wait_recv()
            for j in range(s, s + n):
                cols = slice(j * width, (j + 1) * width)
                total = hold[rows, cols]
                for dx in range(1, nx):
                    total = total + xrcv[dx - 1, r, j].astype(F32)
                out_ref[rows, cols] = total.astype(BF16)

    with jax.named_scope("drain"):
        @pl.when(late)
        def _():
            for copy in swap_qd[:3]:
                copy.wait_send()

        @pl.when(swapping)
        def _():
            for copy in swap_qd[3:]:
                copy.wait_send()
            swap_stats.wait_send()
            remote(dq_send, dq_recv, swap_send.at[group + 1], swap_recv.at[group + 1], ctx=pair).wait_send()

        def fins_sent(z1):
            remote(fsend.at[z1], frcv.at[z1], f_send.at[z1], f_recv.at[z1, 0], ctx=pair).wait_send()

        def drain(z2, _):
            @pl.when(z2 > z)
            def _():
                own_copy(z2).wait_send()

            @pl.when(z2 < z)
            def _():
                fins_sent(z2)
            return 0

        lax.fori_loop(0, zs, drain, 0)

        @pl.when((z == 0) & (y == 0))
        def _():
            pair_own_copy.wait_send()

        @pl.when((z == 0) & (y == 1))
        def _():
            fins_sent(zs - 1)

        remote(w.at[1], w.at[1], w_send.at[0], w_recv.at[0], heads=other).wait_send()
        remote(gs.at[0], gs.at[1], g_send.at[0], g_recv.at[0], heads=other).wait_send()
        for dx in range(1, nx):
            remote(
                xsend.at[dx - 1], xrcv.at[dx - 1], x_send.at[0], x_recv.at[dx - 1, 0], heads=across[dx]
            ).wait_send()


def kernel(zs, nx, ns, group, *refs):
    dma = pltpu.SemaphoreType.DMA
    pl.run_scoped(
        functools.partial(body, zs, nx, ns, *refs),
        in_sem=dma((5,)), w_sem=dma((1,)), w_send=dma((1,)), own_send=dma((zs,)),
        swap_send=dma((group + 2,)), f_send=dma((zs,)), g_send=dma((1,)), x_send=dma((1,)),
    )


def emit(parts, *refs):
    sem = refs[-1]
    copies = []
    for src, dst, n in zip(refs, refs[len(parts):], parts):
        step = src.shape[0] // n
        for i in range(n):
            at = pl.ds(i * step, step)
            copies.append(pltpu.make_async_copy(src.at[at], dst.at[at], sem.at[len(copies)]))
    for copy in copies:
        copy.start()
    for copy in copies:
        copy.wait()


def on_device(
    n, nh, queries, key_states, value_states, attention_out, out_grad, log_sum_exp, block_counts,
    w_query, w_key, w_value,
):
    zs, nx, ns = n // 2, nh // 2, 4
    cap, dim = key_states.shape
    width = queries.shape[1]
    rows = width // dim * cap
    model = w_query.shape[0]
    mine = model // nh
    chunk = mine // ns
    vmem = pl.BlockSpec(memory_space=pltpu.VMEM)
    half = cap // 4
    np = cap // half
    blocks = sum(len(p) for p in row_blocks(np, ns))
    hbm = pl.BlockSpec(memory_space=pltpu.HBM)
    dma = pltpu.SemaphoreType.DMA
    results = pl.pallas_call(
        functools.partial(kernel, zs, nx, ns, width // dim),
        out_shape=(
            jax.ShapeDtypeStruct((cap, mine), BF16),
            jax.ShapeDtypeStruct((cap, dim), F32),
            jax.ShapeDtypeStruct((cap, dim), F32),
        ),
        in_specs=[hbm] * 10,
        out_specs=(vmem, vmem, vmem),
        scratch_shapes=[
            pltpu.SMEM(block_counts.shape, jnp.int32),
            pltpu.VMEM((2, cap, dim), BF16),
            pltpu.VMEM((2, width // dim, 2, cap, dim), BF16),
            pltpu.VMEM((width // dim, cap, dim), BF16),
            pltpu.VMEM(log_sum_exp.shape, F32),
            pltpu.VMEM((2, nx * mine, width + 2 * dim), BF16),
            pltpu.VMEM((2, width + 2 * dim, nx * mine), BF16),
            pltpu.VMEM((2, 2, rows), F32),
            pltpu.VMEM((2, dim, rows), F32),
            pltpu.VMEM((rows, dim), F32),
            pltpu.VMEM((np, width // dim, half, dim), BF16),
            pltpu.VMEM((np, width // dim, half, dim), BF16),
            pltpu.VMEM((2, np, half, width + 2 * dim), BF16),
            pltpu.VMEM((2, cap, dim), F32),
            pltpu.VMEM((zs, 2, cap, dim), BF16),
            pltpu.VMEM((zs, 2, cap, dim), F32),
            pltpu.VMEM((zs, np, 2, half, dim), BF16),
            pltpu.VMEM((zs, np, 2, half, dim), BF16),
            pltpu.VMEM((nx - 1, half, mine), F32),
            pltpu.VMEM((cap, mine), F32),
            pltpu.VMEM((nx - 1, np, ns, half, chunk), BF16),
            pltpu.VMEM((nx - 1, np, ns, half, chunk), BF16),
            dma((1,)),
            dma((zs,)),
            dma((width // dim + 1 + np,)),
            dma((zs, np)),
            dma((np,)),
            dma((nx - 1, blocks)),
            pltpu.SemaphoreType.REGULAR,
        ],
        compiler_params=pltpu.CompilerParams(
            collective_id=0, has_side_effects=True, vmem_limit_bytes=52 * 1024 * 1024
        ),
    )(
        *(
            pltpu.with_memory_space_constraint(a, pltpu.HBM)
            for a in (
                queries, key_states, value_states, attention_out, out_grad, log_sum_exp,
                block_counts, w_query, w_key, w_value,
            )
        )
    )
    return pl.pallas_call(
        functools.partial(emit, (EMIT, 1, 1)),
        out_shape=tuple(jax.ShapeDtypeStruct(a.shape, a.dtype) for a in results),
        in_specs=[vmem] * 3,
        out_specs=(hbm,) * 3,
        scratch_shapes=[dma((EMIT + 2,))],
    )(*(pltpu.with_memory_space_constraint(a, pltpu.VMEM) for a in results))


def solution(mesh):
    return jax.shard_map(
        functools.partial(on_device, mesh.shape["ctx"], mesh.shape["heads"]),
        mesh=mesh,
        in_specs=(
            P("ctx", "heads"),
            P("ctx", "heads"),
            P("ctx", "heads"),
            P("ctx", "heads"),
            P("ctx", "heads"),
            P("heads", "ctx"),
            P(),
            P(None, "heads"),
            P(None, "heads"),
            P(None, "heads"),
        ),
        out_specs=(P("ctx", "heads"), P("ctx", "heads"), P("ctx", "heads")),
        check_vma=False,
    )
```

```python
import functools
import math

import jax
import jax.numpy as jnp
from jax import lax
from jax.experimental import pallas as pl
from jax.experimental.pallas import tpu as pltpu
from jax.sharding import PartitionSpec as P

BLOCK = 64
EMIT = 2
LOG2E = math.log2(math.e)
F32 = jnp.float32
BF16 = jnp.bfloat16
NT = (((1,), (1,)), ((), ()))
TN = (((0,), (0,)), ((), ()))


def dot(a, b, dims=(((1,), (0,)), ((), ()))):
    return lax.dot_general(a, b, dims, preferred_element_type=F32)


def row_blocks(np, ns):
    plan = []
    for r in range(np):
        if r == 0:
            plan.append(((0, 1), (1, 1), (2, ns - 2)))
        elif r == np - 1:
            plan.append(((0, ns - 2), (ns - 2, 1), (ns - 1, 1)))
        else:
            plan.append(((0, ns // 2), (ns // 2, ns - ns // 2)))
    return plan


def body(
    zs, nx, ns,
    q_hbm, k_hbm, v_hbm, o_hbm, do_hbm, lse_hbm, cnt_hbm, wq_hbm, wk_hbm, wv_hbm,
    out_ref, dk_ref, dv_ref,
    cnt_ref, own, qd, o_ref, lse_ref, w, wt, stats, dqt,
    dq_own, dq_send, dq_recv, gs, acc, kv, part, fsend, frcv, keep, hold, xsend, xrcv,
    w_recv, kv_recv, swap_recv, f_recv, g_recv, x_recv, turn,
    in_sem, w_sem, w_send, own_send, swap_send, f_send, g_send, x_send,
):
    cap, dim = own.shape[1:]
    group = qd.shape[1]
    np = dq_send.shape[0]
    half = cap // np
    scale = 1.0 / math.sqrt(dim)
    plan = row_blocks(np, ns)
    first = [sum(len(p) for p in plan[:r]) for r in range(np)]
    me = lax.axis_index("ctx")
    y = lax.rem(me, 2)
    z = lax.div(me, 2)
    pair = me + 1 - 2 * y
    h = lax.axis_index("heads")
    core = lax.rem(h, 2)
    x = lax.div(h, 2)
    other = h + 1 - 2 * core
    across = [h] + [2 * lax.rem(x + dx, nx) + 1 - core for dx in range(1, nx)]
    theirs = [other] + [2 * lax.rem(x + dx, nx) + core for dx in range(1, nx)]

    def remote(src, dst, send, recv, **device):
        return pltpu.make_async_remote_copy(
            src_ref=src, dst_ref=dst, send_sem=send, recv_sem=recv,
            device_id=device, device_id_type=pl.DeviceIdType.MESH,
        )

    mine = w.shape[1] // nx
    wide = group * dim
    weights = ((wq_hbm, 0, wide), (wk_hbm, wide, dim), (wv_hbm, wide + dim, dim))

    def w_rows(owner, src):
        return src.at[pl.ds(pl.multiple_of(owner * mine, mine), mine), :]

    w_loads = [
        pltpu.make_async_copy(
            w_rows(across[dx], src), w.at[0, pl.ds(dx * mine, mine), pl.ds(at, size)], w_sem.at[0]
        )
        for dx in range(nx)
        for src, at, size in weights
    ]
    w_shares = [
        remote(
            w_rows(theirs[dx], src), w.at[1, pl.ds(dx * mine, mine), pl.ds(at, size)],
            w_send.at[0], w_recv.at[0], heads=other,
        )
        for dx in range(nx)
        for src, at, size in weights
    ]
    barrier = pltpu.get_barrier_semaphore()

    def greet(**device):
        pl.semaphore_signal(
            barrier, inc=1, device_id=device, device_id_type=pl.DeviceIdType.MESH
        )

    def greet_line(z2, _):
        @pl.when(z2 != z)
        def _():
            greet(ctx=2 * z2 + y)
        return 0

    lax.fori_loop(0, zs, greet_line, 0)
    greet(ctx=pair)
    greet(heads=other)
    for dx in range(1, nx):
        greet(heads=across[dx])

    heads = [pl.ds(g * dim, dim) for g in range(group)]
    loads = [
        pltpu.make_async_copy(src, dst, in_sem.at[i])
        for src, dst, i in (
            (k_hbm, own.at[0], 0), (v_hbm, own.at[1], 0),
            *((q_hbm.at[:, heads[g]], qd.at[0, g, 0], 1) for g in range(group)),
            *((do_hbm.at[:, heads[g]], qd.at[0, g, 1], 1) for g in range(group)),
            *((o_hbm.at[:, heads[g]], o_ref.at[g], 2) for g in range(group)),
            (lse_hbm, lse_ref, 3), (cnt_hbm, cnt_ref, 4),
        )
    ]
    for copy in loads:
        copy.start()
    pltpu.make_async_copy(own, own, in_sem.at[0]).wait()
    pltpu.make_async_copy(qd.at[0], qd.at[0], in_sem.at[1]).wait()
    pltpu.make_async_copy(o_ref, o_ref, in_sem.at[2]).wait()
    for copy in loads[-2:]:
        copy.wait()
    for copy in w_loads:
        copy.start()
    with jax.named_scope("barrier"):
        pl.semaphore_wait(barrier, zs + nx)

    def own_copy(z2):
        return remote(own, kv.at[z], own_send.at[z2], kv_recv.at[z], ctx=2 * z2 + y)

    pair_own_copy = remote(own, kv.at[zs - 1], own_send.at[0], kv_recv.at[zs - 1], ctx=pair)

    def arrived(z1):
        remote(kv.at[z1], kv.at[z1], own_send.at[z1], kv_recv.at[z1], ctx=pair).wait_recv()

    swap_qd = [
        remote(qd.at[0, g], qd.at[1, g], swap_send.at[g], swap_recv.at[0], ctx=pair)
        for g in range(group)
    ]
    swap_stats = remote(
        stats.at[0], stats.at[1], swap_send.at[group], swap_recv.at[1], ctx=pair
    )

    def swap_dq(r):
        return remote(
            dq_send.at[r], dq_recv.at[r], swap_send.at[group + 1], swap_recv.at[2 + r], ctx=pair
        )

    def fin_copy(r, z1):
        return remote(
            fsend.at[z1, r], frcv.at[z, r], f_send.at[z1], f_recv.at[z, r], ctx=2 * z1 + y
        )

    def pair_fin(r):
        return remote(
            fsend.at[zs - 1, r], frcv.at[0, r], f_send.at[zs - 1], f_recv.at[0, r], ctx=pair
        )

    def fin_wait(r, z2):
        remote(
            fsend.at[z2, r], frcv.at[z2, r], f_send.at[z2], f_recv.at[z2, r], ctx=pair
        ).wait_recv()

    swapping = z > 0
    early = swapping & (core == 0)
    late = swapping & (core == 1)

    @pl.when(early)
    def _():
        for copy in swap_qd:
            copy.start()

    @pl.when((z == 0) & (y == 0))
    def _():
        pair_own_copy.start()

    def push_own(i, _):
        z2 = zs - 1 - i

        @pl.when(z2 > z)
        def _():
            own_copy(z2).start()
        return 0

    lax.fori_loop(0, zs, push_own, 0)

    lane = lax.broadcasted_iota(jnp.int32, (1, group * cap), 1)
    row = lax.rem(lane, cap)
    alive = row < cnt_ref[me] * BLOCK
    def flat(ref):
        return ref[...].reshape(group * cap, dim)

    prod = flat(qd.at[0, :, 1]).astype(F32) * flat(o_ref).astype(F32)
    stats[0, 1:2] = lax.dot_general(
        jnp.ones((8, dim), F32), prod, NT,
        preferred_element_type=F32, precision=lax.Precision.HIGHEST,
    )[0:1]
    lse_row = jnp.concatenate([lse_ref[g:g + 1, :] for g in range(group)], axis=1)
    stats[0, 0:1] = jnp.where(alive, lse_row * LOG2E, 1e30)

    @pl.when(swapping)
    def _():
        swap_stats.start()

    key_row = lax.broadcasted_iota(jnp.int32, (cap, group * cap), 0)

    def products(key, value, query, out_grad, lse, delta, visible):
        scores = dot(key, query, NT)
        prob_grad = dot(value, out_grad, NT)
        prob = jnp.where(visible, jnp.exp2(scores * (scale * LOG2E) - lse), 0.0)
        grad = (prob * (prob_grad - delta)).astype(BF16)
        return dot(grad, query), dot(prob.astype(BF16), out_grad), dot(key, grad, TN)

    def tile(who, key, value, b, diagonal):
        visible = key_row < cnt_ref[b] * BLOCK
        if diagonal:
            visible = visible & (key_row <= row)
        d_key, d_value, terms = products(
            key, value, flat(qd.at[who, :, 0]), flat(qd.at[who, :, 1]),
            stats[who, 0:1], stats[who, 1:2], visible,
        )
        if diagonal:
            dqt[who] = terms
        else:
            dqt[who] += terms
        return d_key, d_value

    with jax.named_scope("diag"):
        d_key, d_value = tile(0, own[0], own[1], me, True)
        acc[0] = d_key
        acc[1] = d_value

    for copy in w_shares:
        copy.start()

    @pl.when(early)
    def _():
        with jax.named_scope("hand_over"):
            for copy in swap_qd[:3]:
                copy.wait_send()
            pl.semaphore_signal(
                turn, inc=1, device_id={"heads": other}, device_id_type=pl.DeviceIdType.MESH
            )

    @pl.when(late)
    def _():
        with jax.named_scope("my_turn"):
            pl.semaphore_wait(turn, 1)
            for copy in swap_qd:
                copy.start()

    def turn_w(c):
        def step(i, _):
            at = pl.ds(pl.multiple_of(i * 256, 256), 256)
            wt[c, :, at] = jnp.transpose(w[c, at, :])
            return 0
        with jax.named_scope("turn_w"):
            lax.fori_loop(0, w.shape[1] // 256, step, 0)

    pltpu.make_async_copy(w.at[0], w.at[0], w_sem.at[0]).wait()
    turn_w(0)

    def ship(z1, d_key, d_value, pieces):
        for r in pieces:
            fsend[z1, r, 0] = d_key[r * half:(r + 1) * half].astype(BF16)
            fsend[z1, r, 1] = d_value[r * half:(r + 1) * half].astype(BF16)

    def later(pieces):
        def step(z1, _):
            for r in pieces:
                sent = ((z1 == 0) & (early | ((z > 1) if r == 1 else False))) if r < np - 1 else z1 < 0

                @pl.when((z1 < z) & jnp.logical_not(sent))
                def _():
                    fin_copy(r, z1).start()
            return 0
        lax.fori_loop(0, zs, step, 0)

    def last_pieces():
        later([np - 1])

    def swapped():
        dqt[1] = jnp.zeros_like(dqt[1])
        with jax.named_scope("wait_swap"):
            swap_stats.wait_recv()
            remote(qd.at[0], qd.at[1], swap_send.at[0], swap_recv.at[0], ctx=pair).wait_recv()

    def leave(z1, d_key, d_value):
        ship(z1, d_key, d_value, range(1))
        fin_copy(0, z1).start()
        ship(z1, d_key, d_value, range(1, np))

    def pair_tile(z1):
        with jax.named_scope("pair_tile"):
            d_key, d_value = tile(1, kv[z1, 0], kv[z1, 1], 2 * z1 + y, False)
            leave(z1, part[z1, 0] + d_key, part[z1, 1] + d_value)

        @pl.when(((z1 == 0) & early) | ((z1 == 1) & late))
        def _():
            fin_copy(1, 0).start()

        @pl.when((z1 == 0) & early)
        def _():
            for r in range(2, np - 1):
                fin_copy(r, 0).start()

    def own_step(z1, _):
        @pl.when((z1 < z) | ((z1 == zs - 1) & (z == 0) & (y == 1)))
        def _():
            with jax.named_scope("wait_kv"):
                arrived(z1)
            with jax.named_scope("own_tile"):
                b = jnp.where(z == 0, pair, 2 * z1 + y)
                d_key, d_value = tile(0, kv[z1, 0], kv[z1, 1], b, False)
                part[z1, 0] = d_key
                part[z1, 1] = d_value

        pl.when((z1 == 0) & early)(swapped)

        @pl.when((z1 < z) & early)
        def _():
            pair_tile(z1)
        return 0

    lax.fori_loop(0, zs, own_step, 0)

    @pl.when(early)
    def _():
        later(range(1, np - 1))
        pl.when(z == zs - 1)(last_pieces)

    @pl.when((z == 0) & (y == 1))
    def _():
        ship(zs - 1, part[zs - 1, 0], part[zs - 1, 1], range(np))
        for r in range(np):
            pair_fin(r).start()

    @pl.when(z == 0)
    def _():
        dq_recv[...] = jnp.zeros_like(dq_recv)

    dq_own[...] = jnp.transpose(dqt[0])

    @pl.when(late)
    def _():
        swapped()

        def pair_step(z1, _):
            @pl.when(z1 < z)
            def _():
                pair_tile(z1)
            return 0

        lax.fori_loop(0, zs, pair_step, 0)
        later(range(1, np - 1))
        pl.when(z == zs - 1)(last_pieces)

    @pl.when(swapping & (y == 0))
    def _():
        with jax.named_scope("pair_own"):
            d_key, d_value = tile(1, own[0], own[1], me, False)
            acc[0] += d_key
            acc[1] += d_value

    @pl.when(swapping)
    def _():
        pair_dq = jnp.transpose(dqt[1]).astype(BF16)
        for r in range(np):
            for g in range(group):
                dq_send[r, g] = pair_dq[g * cap + r * half:g * cap + (r + 1) * half]
            swap_dq(r).start()

    width = mine // ns

    def g_copy(r, at=0, size=None):
        columns = pl.ds(at, wide + 2 * dim if size is None else size)
        return remote(
            gs.at[0, r, :, columns], gs.at[1, r, :, columns], g_send.at[0], g_recv.at[r], heads=other
        )

    def side(c, dx, s, n, r):
        cols = slice(dx * mine + s * width, dx * mine + (s + n) * width)
        return dot(gs[c, r], wt[c, :, cols])

    def whole(dx, s, n, r):
        return side(0, dx, s, n, r) + side(1, dx, s, n, r)

    def cross_copy(dx, r, i):
        at = (dx - 1, r, pl.ds(*plan[r][i]))
        return remote(
            xsend.at[at], xrcv.at[at], x_send.at[0], x_recv.at[dx - 1, r + i * (r == np - 1)], heads=across[dx]
        )

    remote(w.at[1], w.at[1], w_send.at[0], w_recv.at[0], heads=other).wait_recv()
    turn_w(1)

    for r in range(np):
        rows = slice(r * half, (r + 1) * half)

        def collect(z2, _):
            @pl.when((z2 > z) | ((z2 == 0) & (z == 0) & (y == 0)))
            def _():
                fin_wait(r, z2)
                acc[:, rows, :] += frcv[z2, r].astype(F32)
            return 0

        with jax.named_scope("wait_dq"):
            @pl.when(swapping)
            def _():
                swap_dq(r).wait_recv()
        if r == 0:
            pl.when(z < zs - 1)(last_pieces)
        for g in range(group):
            total = dq_own[g * cap + r * half:g * cap + (r + 1) * half, :] + dq_recv[r, g].astype(F32)
            gs[0, r, :, g * dim:(g + 1) * dim] = (total * scale).astype(BF16)
        g_copy(r, 0, wide).start()
        with jax.named_scope("collect"):
            lax.fori_loop(0, zs, collect, 0)
        key_total = acc[0, rows, :] * scale
        value_total = acc[1, rows, :]
        gs[0, r, :, wide:wide + dim] = key_total.astype(BF16)
        gs[0, r, :, wide + dim:wide + 2 * dim] = value_total.astype(BF16)
        g_copy(r, wide, 2 * dim).start()
        dk_ref[rows, :] = key_total
        dv_ref[rows, :] = value_total
        blocks = [(dx, i) for dx in range(1, nx) for i in range(len(plan[r]))]

        def half_sum(dx, i):
            s, n = plan[r][i]
            keep[dx - 1, :, s * width:(s + n) * width] = side(0, dx, s, n, r)

        def finish(dx, i):
            s, n = plan[r][i]
            terms = keep[dx - 1, :, s * width:(s + n) * width] + side(1, dx, s, n, r)
            terms = terms.astype(BF16)
            for j in range(n):
                xsend[dx - 1, r, s + j] = terms[:, j * width:(j + 1) * width]
            cross_copy(dx, r, i).start()

        def waiting():
            with jax.named_scope("half"):
                for dx, i in blocks:
                    half_sum(dx, i)
            with jax.named_scope("wait_g"):
                g_copy(r).wait_recv()
            with jax.named_scope("project"):
                for dx, i in blocks:
                    finish(dx, i)

        def ready():
            with jax.named_scope("wait_g"):
                g_copy(r).wait_recv()
            with jax.named_scope("project"):
                for dx, i in blocks:
                    half_sum(dx, i)
                    finish(dx, i)

        if r == 0:
            pl.when(core == 0)(waiting)
            pl.when(core == 1)(ready)
        else:
            waiting()
    with jax.named_scope("own_proj"):
        for r in range(np):
            for s in range(0, ns, 2):
                hold[r * half:(r + 1) * half, s * width:(s + 2) * width] = whole(0, s, 2, r)
    for r in range(np):
        rows = slice(r * half, (r + 1) * half)
        for i, (s, n) in enumerate(plan[r]):
            for dx in range(1, nx):
                with jax.named_scope("wait_cross"):
                    if r == np - 1:
                        cross_copy(dx, r, i).wait_recv()
                    elif i == 0:
                        remote(
                            xsend.at[dx - 1, r], xrcv.at[dx - 1, r], x_send.at[0], x_recv.at[dx - 1, r],
                            heads=across[dx],
                        ).wait_recv()
            for j in range(s, s + n):
                cols = slice(j * width, (j + 1) * width)
                total = hold[rows, cols]
                for dx in range(1, nx):
                    total = total + xrcv[dx - 1, r, j].astype(F32)
                out_ref[rows, cols] = total.astype(BF16)

    with jax.named_scope("drain"):
        @pl.when(late)
        def _():
            for copy in swap_qd[:3]:
                copy.wait_send()

        @pl.when(swapping)
        def _():
            for copy in swap_qd[3:]:
                copy.wait_send()
            swap_stats.wait_send()
            remote(dq_send, dq_recv, swap_send.at[group + 1], swap_recv.at[2], ctx=pair).wait_send()

        def fins_sent(z1):
            remote(fsend.at[z1], frcv.at[z1], f_send.at[z1], f_recv.at[z1, 0], ctx=pair).wait_send()

        def drain(z2, _):
            @pl.when(z2 > z)
            def _():
                own_copy(z2).wait_send()

            @pl.when(z2 < z)
            def _():
                fins_sent(z2)
            return 0

        lax.fori_loop(0, zs, drain, 0)

        @pl.when((z == 0) & (y == 0))
        def _():
            pair_own_copy.wait_send()

        @pl.when((z == 0) & (y == 1))
        def _():
            fins_sent(zs - 1)

        remote(w.at[1], w.at[1], w_send.at[0], w_recv.at[0], heads=other).wait_send()
        remote(gs.at[0], gs.at[1], g_send.at[0], g_recv.at[0], heads=other).wait_send()
        for dx in range(1, nx):
            remote(
                xsend.at[dx - 1], xrcv.at[dx - 1], x_send.at[0], x_recv.at[dx - 1, 0], heads=across[dx]
            ).wait_send()


def kernel(zs, nx, ns, group, *refs):
    dma = pltpu.SemaphoreType.DMA
    pl.run_scoped(
        functools.partial(body, zs, nx, ns, *refs),
        in_sem=dma((5,)), w_sem=dma((1,)), w_send=dma((1,)), own_send=dma((zs,)),
        swap_send=dma((group + 2,)), f_send=dma((zs,)), g_send=dma((1,)), x_send=dma((1,)),
    )


def emit(parts, *refs):
    sem = refs[-1]
    copies = []
    for src, dst, n in zip(refs, refs[len(parts):], parts):
        step = src.shape[0] // n
        for i in range(n):
            at = pl.ds(i * step, step)
            copies.append(pltpu.make_async_copy(src.at[at], dst.at[at], sem.at[len(copies)]))
    for copy in copies:
        copy.start()
    for copy in copies:
        copy.wait()


def on_device(
    n, nh, queries, key_states, value_states, attention_out, out_grad, log_sum_exp, block_counts,
    w_query, w_key, w_value,
):
    zs, nx, ns = n // 2, nh // 2, 4
    cap, dim = key_states.shape
    width = queries.shape[1]
    rows = width // dim * cap
    model = w_query.shape[0]
    mine = model // nh
    chunk = mine // ns
    vmem = pl.BlockSpec(memory_space=pltpu.VMEM)
    half = cap // 4
    np = cap // half
    blocks = np - 1 + len(row_blocks(np, ns)[-1])
    hbm = pl.BlockSpec(memory_space=pltpu.HBM)
    dma = pltpu.SemaphoreType.DMA
    results = pl.pallas_call(
        functools.partial(kernel, zs, nx, ns, width // dim),
        out_shape=(
            jax.ShapeDtypeStruct((cap, mine), BF16),
            jax.ShapeDtypeStruct((cap, dim), F32),
            jax.ShapeDtypeStruct((cap, dim), F32),
        ),
        in_specs=[hbm] * 10,
        out_specs=(vmem, vmem, vmem),
        scratch_shapes=[
            pltpu.SMEM(block_counts.shape, jnp.int32),
            pltpu.VMEM((2, cap, dim), BF16),
            pltpu.VMEM((2, width // dim, 2, cap, dim), BF16),
            pltpu.VMEM((width // dim, cap, dim), BF16),
            pltpu.VMEM(log_sum_exp.shape, F32),
            pltpu.VMEM((2, nx * mine, width + 2 * dim), BF16),
            pltpu.VMEM((2, width + 2 * dim, nx * mine), BF16),
            pltpu.VMEM((2, 2, rows), F32),
            pltpu.VMEM((2, dim, rows), F32),
            pltpu.VMEM((rows, dim), F32),
            pltpu.VMEM((np, width // dim, half, dim), BF16),
            pltpu.VMEM((np, width // dim, half, dim), BF16),
            pltpu.VMEM((2, np, half, width + 2 * dim), BF16),
            pltpu.VMEM((2, cap, dim), F32),
            pltpu.VMEM((zs, 2, cap, dim), BF16),
            pltpu.VMEM((zs, 2, cap, dim), F32),
            pltpu.VMEM((zs, np, 2, half, dim), BF16),
            pltpu.VMEM((zs, np, 2, half, dim), BF16),
            pltpu.VMEM((nx - 1, half, mine), F32),
            pltpu.VMEM((cap, mine), F32),
            pltpu.VMEM((nx - 1, np, ns, half, chunk), BF16),
            pltpu.VMEM((nx - 1, np, ns, half, chunk), BF16),
            dma((1,)),
            dma((zs,)),
            dma((2 + np,)),
            dma((zs, np)),
            dma((np,)),
            dma((nx - 1, blocks)),
            pltpu.SemaphoreType.REGULAR,
        ],
        compiler_params=pltpu.CompilerParams(
            collective_id=0, has_side_effects=True, vmem_limit_bytes=52 * 1024 * 1024
        ),
    )(
        *(
            pltpu.with_memory_space_constraint(a, pltpu.HBM)
            for a in (
                queries, key_states, value_states, attention_out, out_grad, log_sum_exp,
                block_counts, w_query, w_key, w_value,
            )
        )
    )
    return pl.pallas_call(
        functools.partial(emit, (EMIT, 1, 1)),
        out_shape=tuple(jax.ShapeDtypeStruct(a.shape, a.dtype) for a in results),
        in_specs=[vmem] * 3,
        out_specs=(hbm,) * 3,
        scratch_shapes=[dma((EMIT + 2,))],
    )(*(pltpu.with_memory_space_constraint(a, pltpu.VMEM) for a in results))


def solution(mesh):
    return jax.shard_map(
        functools.partial(on_device, mesh.shape["ctx"], mesh.shape["heads"]),
        mesh=mesh,
        in_specs=(
            P("ctx", "heads"),
            P("ctx", "heads"),
            P("ctx", "heads"),
            P("ctx", "heads"),
            P("ctx", "heads"),
            P("heads", "ctx"),
            P(),
            P(None, "heads"),
            P(None, "heads"),
            P(None, "heads"),
        ),
        out_specs=(P("ctx", "heads"), P("ctx", "heads"), P("ctx", "heads")),
        check_vma=False,
    )
```
